32 devices in a mesh: seq: 8 (over z, x), head: 4 (over y, core).
Axes of the slice: x: 2, y: 2, z: 4, core: 2. Of those that a mesh axis runs over, the one named last changes fastest.
Arguments:
- queries: bfloat16 [2048, 4096], P('seq', 'head'), may hold values from -6 to 6
- keys: bfloat16 [2048, 4096], P('seq', 'head'), may hold values from -6 to 6
- values: bfloat16 [2048, 4096], P('seq', 'head'), may hold values from -6 to 6
- outputs: bfloat16 [2048, 4096], P('seq', 'head'), may hold values from -6 to 6
- out_grad: bfloat16 [2048, 4096], P('seq', 'head'), may hold values from -6 to 6
- log_sum: float32 [32, 2048], P('head', 'seq'), may hold values from 4 to 6
- selected: int32 [32, 32, 16], P('head', 'seq'), may hold values from -1 to 31, as said below
- w_query: bfloat16 [4096, 4096], P(None, 'head'), may hold values from -0.09375 to 0.09375
Outputs:
- x_grad: bfloat16 [2048, 4096], P(('seq', 'head'))
- key_gradient: bfloat16 [2048, 4096], P('seq', 'head')
- value_gradient: bfloat16 [2048, 4096], P('seq', 'head')
The draws below stay inside these ranges and needn't reach their ends.
Inputs may be any that keep to these rules, and one draw needn't show every extreme that they name: Row (h, b) lists distinct blocks: entry 0 is b itself, the others are blocks before b, and entries equal to -1 (unused) come last. Over the query blocks of one index of seq and the heads of one index of head, the distinct (head, block) pairs selected from the blocks of any one other index of seq number at most 2; some pair of indices reaches 2 in every draw.
All inputs are finite; a program needn't handle non-finite values.
Results may differ from the reference program's by a relative error of at most 0.0075.
Values may be sent and summed in bfloat16 or wider, within the bound.
No kernel may reach another device: no remote copies, remote signals or barrier semaphores. Data moves between devices by JAX's collectives and lax.ppermute only.
A program may use at most 128 MiB of HBM per device.

```python
import jax
import jax.numpy as jnp
from jax import lax

DWIN = 4096
HEADS_DEV = 8
HD = 128
BLOCK = 64
TOPK = 16
CAP = 2
BLK_DEV = 4
TOKENS = 2048
NQB = 32
HEADS = 32


def draw_selected(key, part):
    shards = NQB // BLK_DEV
    groups = HEADS // HEADS_DEV
    pick_count = TOPK - 1
    score_span = 1 << 16
    key_order, key_offset, key_pick = jax.random.split(jax.random.fold_in(key, 7), 3)
    requester = jnp.arange(shards, dtype=jnp.int32)
    ranking = jax.random.randint(key_order, (groups, shards, shards), 0, score_span) * shards + requester[None, None, :]
    ranking = jnp.where(requester[None, None, :] < requester[None, :, None], ranking, ranking + score_span * shards)
    ranking = jnp.argsort(ranking, axis=-1, stable=True).astype(jnp.int32)
    remote_count = jnp.minimum(pick_count, CAP * requester // HEADS_DEV)
    head_local = jnp.arange(HEADS_DEV, dtype=jnp.int32)
    column = jnp.arange(pick_count, dtype=jnp.int32)
    slot_number = head_local[None, :, None] * remote_count[:, None, None] + column[None, None, :]
    slot_number = jnp.minimum(slot_number, shards * CAP - 1)
    lookup = jnp.broadcast_to((slot_number // CAP).reshape(1, shards, -1), (groups, shards, HEADS_DEV * pick_count))
    source = jnp.take_along_axis(ranking, lookup, axis=2)
    offset = jax.random.randint(key_offset, (groups, shards, shards), 0, BLK_DEV)
    offset = jnp.take_along_axis(offset, source, axis=2).reshape(groups, shards, HEADS_DEV, pick_count)
    source = source.reshape(groups, shards, HEADS_DEV, pick_count)
    remote_block = source * BLK_DEV + (offset + slot_number[None] % CAP) % BLK_DEV
    remote_valid = jnp.broadcast_to((column[None, :] < remote_count[:, None])[None, :, None, :], remote_block.shape)
    inner = jnp.arange(BLK_DEV, dtype=jnp.int32)
    earlier = jnp.arange(BLK_DEV - 1, dtype=jnp.int32)
    local_block = requester[:, None, None] * BLK_DEV + earlier[None, None, :] + 0 * inner[None, :, None]
    local_valid = earlier[None, :] < inner[:, None]
    full_shape = (groups, shards, HEADS_DEV, BLK_DEV)
    candidate = jnp.concatenate((jnp.broadcast_to(remote_block[:, :, :, None, :], full_shape + (pick_count,)), jnp.broadcast_to(local_block[None, :, None, :, :], full_shape + (BLK_DEV - 1,))), axis=-1)
    usable = jnp.concatenate((jnp.broadcast_to(remote_valid[:, :, :, None, :], full_shape + (pick_count,)), jnp.broadcast_to(local_valid[None, None, None, :, :], full_shape + (BLK_DEV - 1,))), axis=-1)
    width_all = pick_count + BLK_DEV - 1
    shuffle = jax.random.randint(key_pick, candidate.shape, 0, score_span) * width_all + jnp.arange(width_all, dtype=jnp.int32)
    shuffle = jnp.where(usable, shuffle, shuffle + score_span * width_all)
    picked = jnp.argsort(shuffle, axis=-1, stable=True)[..., :pick_count]
    chosen = jnp.take_along_axis(candidate, picked, axis=-1)
    chosen_valid = jnp.take_along_axis(usable, picked, axis=-1)
    chosen = jnp.where(chosen_valid, chosen, -1)
    own_block = jnp.broadcast_to((requester[:, None] * BLK_DEV + inner[None, :])[None, :, None, :, None], full_shape + (1,))
    selection = jnp.concatenate((own_block, chosen), axis=-1)
    selection = selection.transpose(0, 2, 1, 3, 4).reshape(HEADS, NQB, TOPK)
    return selection.astype(jnp.int32)


def shard_levels(rng, shape, cuts, low, top_value):
    level = 1.0
    for axis_at, blocks in cuts:
        steps = jax.random.uniform(jax.random.fold_in(jax.random.fold_in(rng, 6), axis_at), (blocks,), jnp.float32, low / len(cuts), top_value / len(cuts))
        level = level * jnp.repeat(jnp.exp(steps), shape[axis_at] // blocks).reshape((-1,) + (1,) * (len(shape) - 1 - axis_at))
    return level


def normal_values(stream_key, extent, scale, limit, cuts=(), kind=jnp.bfloat16):
    loudness = shard_levels(stream_key, extent, cuts, -0.22, 0.18) if cuts else 1.0
    array = jax.random.normal(stream_key, extent, jnp.float32) * scale * loudness
    return jnp.minimum(jnp.maximum(array, -limit), limit).astype(kind)


def setup_inputs(seed: int = 0) -> dict:
    streams_of = jax.random.split(jax.random.key(seed), 9)
    return {
        "queries": normal_values(streams_of[0], (TOKENS, HEADS * HD), 1.0, 6.0, ((0, 8), (1, 4))),
        "keys": normal_values(streams_of[1], (TOKENS, HEADS * HD), 1.0, 6.0, ((0, 8), (1, 4))),
        "values": normal_values(streams_of[2], (TOKENS, HEADS * HD), 1.0, 6.0, ((0, 8), (1, 4))),
        "outputs": normal_values(streams_of[3], (TOKENS, HEADS * HD), 1.0, 6.0, ((0, 8), (1, 4))),
        "out_grad": normal_values(streams_of[4], (TOKENS, HEADS * HD), 1.0, 6.0, ((0, 8), (1, 4))),
        "log_sum": jnp.clip(4.0 + 2.0 * jax.random.uniform(streams_of[5], (HEADS, TOKENS), jnp.float32) ** shard_levels(streams_of[5], (HEADS, TOKENS), ((0, 4), (1, 8)), -0.2, 0.2), 4.0, 6.0),
        "selected": draw_selected(jax.random.fold_in(streams_of[8], 71), 0),
        "w_query": normal_values(streams_of[7], (DWIN, HEADS * HD), (HEADS * HD) ** -0.5, 0.09375, ((1, 4),)),
    }


def reference(queries, keys, values, outputs, out_grad, log_sum, selected, w_query):
    logit_scale = HD ** -0.5
    offsets = jnp.arange(BLOCK, dtype=jnp.int32)
    query_pos = jnp.arange(NQB, dtype=jnp.int32)[:, None] * BLOCK + offsets[None, :]

    def one_head(head_number):
        def columns(matrix):
            part = lax.dynamic_slice_in_dim(matrix, head_number * HD, HD, 1)
            return part.astype(jnp.float32).reshape(NQB, BLOCK, HD)

        query_slice = columns(queries)
        key_part = columns(keys)
        value_part = columns(values)
        partial_gradient = columns(out_grad)
        out_part = columns(outputs)
        log_part = lax.dynamic_index_in_dim(log_sum, head_number, 0, False).reshape(NQB, BLOCK)
        chosen = lax.dynamic_index_in_dim(selected, head_number, 0, False)
        safe = jnp.maximum(chosen, 0).astype(jnp.int32)
        selected_keys = key_part[safe]
        selected_values = value_part[safe]
        delta = jnp.sum(partial_gradient * out_part, axis=-1)
        attention_logits = jnp.einsum("wyj,wcmj->wycm", query_slice, selected_keys) * logit_scale
        key_pos = chosen[:, None, :, None] * BLOCK + offsets[None, None, None, :]
        allowed = (chosen >= 0)[:, None, :, None] & (key_pos <= query_pos[:, :, None, None])
        probs = jnp.where(allowed, jnp.exp(attention_logits - log_part[:, :, None, None]), jnp.float32(0.0))
        reduced_probabilities = lax.optimization_barrier(probs.astype(jnp.bfloat16)).astype(jnp.float32)
        probability_gradient = jnp.einsum("wyj,wcmj->wycm", partial_gradient, selected_values)
        score_gradient = probs * (probability_gradient - delta[:, :, None, None])
        score_gradient = lax.optimization_barrier(score_gradient.astype(jnp.bfloat16)).astype(jnp.float32)
        query_gradient = jnp.einsum("gwfp,gfpe->gwe", score_gradient, selected_keys) * logit_scale
        key_gradient = jnp.einsum("unye,unv->uyev", score_gradient, query_slice) * logit_scale
        value_gradient = jnp.einsum("unye,unv->uyev", reduced_probabilities, partial_gradient)
        both = jnp.concatenate((key_gradient, value_gradient), axis=-1)
        totals = jnp.zeros((NQB, BLOCK, 2 * HD), jnp.float32).at[safe].add(both)
        return query_gradient.astype(jnp.bfloat16), totals

    query_grads, totals = lax.map(one_head, jnp.arange(HEADS, dtype=jnp.int32))
    query_rows = query_grads.reshape(HEADS, TOKENS, HD).transpose(1, 0, 2).reshape(TOKENS, HEADS * HD)
    x_grad = jnp.dot(query_rows, w_query.T, preferred_element_type=jnp.float32).astype(jnp.bfloat16)
    arranged = totals.reshape(HEADS, TOKENS, 2 * HD).transpose(1, 0, 2)
    key_gradient = arranged[:, :, :HD].reshape(TOKENS, HEADS * HD).astype(jnp.bfloat16)
    value_gradient = arranged[:, :, HD:].reshape(TOKENS, HEADS * HD).astype(jnp.bfloat16)
    return (x_grad, key_gradient, value_gradient)
```

```python
import functools

import jax
import jax.numpy as jnp
from jax import lax
from jax.experimental import pallas as pl
from jax.experimental.pallas import tpu as pltpu
from jax.sharding import PartitionSpec as P

CAP = 2
LANES = 128
FAR = 1e30
NONE = 1 << 20

VMEM = pl.BlockSpec(memory_space=pltpu.VMEM)
SMEM = pl.BlockSpec(memory_space=pltpu.SMEM)


def dot_nt(a, b, precision=None):
    return lax.dot_general(
        a, b, (((1,), (1,)), ((), ())), preferred_element_type=jnp.float32, precision=precision
    )


def dot_nn(a, b):
    return lax.dot_general(a, b, (((1,), (0,)), ((), ())), preferred_element_type=jnp.float32)


def dot_tn(a, b):
    return lax.dot_general(a, b, (((0,), (0,)), ((), ())), preferred_element_type=jnp.float32)


def index_kernel(shards, selected_ref, wanted_ref, bits_ref):
    head_count, block_count, pick_count = selected_ref.shape
    width = bits_ref.shape[1]
    me = lax.axis_index("seq")
    lane = lax.broadcasted_iota(jnp.int32, (block_count, width), 1)
    weight = jnp.left_shift(1, lax.broadcasted_iota(jnp.int32, (block_count, width), 0))
    for head in range(head_count):
        rows = selected_ref[head]
        hits = jnp.zeros((block_count, width), jnp.int32)
        for pick in range(pick_count):
            hits = jnp.where(rows[:, pick : pick + 1] == lane, weight, hits)
        bits_ref[head : head + 1, :] = jnp.sum(hits, axis=0, keepdims=True)
    bits = bits_ref[...]
    lane = lax.broadcasted_iota(jnp.int32, (head_count, width), 1)
    label = lax.broadcasted_iota(jnp.int32, (head_count, width), 0) * block_count + lax.rem(
        lane, block_count
    )
    label = jnp.where((bits > 0) & (lax.div(lane, block_count) != me), label, NONE)
    owner_lane = lax.div(lax.broadcasted_iota(jnp.int32, (shards, width), 1), block_count)
    mine = owner_lane == lax.broadcasted_iota(jnp.int32, (shards, width), 0)
    column = lax.broadcasted_iota(jnp.int32, (shards, LANES), 1)
    wanted = jnp.full((shards, LANES), -1, jnp.int32)
    for slot in range(CAP):
        lowest = jnp.min(label, axis=0, keepdims=True)
        slot_value = jnp.min(jnp.where(mine, lowest, NONE), axis=1, keepdims=True)
        wanted = jnp.where((column == slot) & (slot_value < NONE), slot_value, wanted)
        taken = jnp.min(jnp.where(mine, slot_value, NONE), axis=0, keepdims=True)
        label = jnp.where(label == taken, NONE, label)
    for owner in range(shards):
        wanted_ref[owner] = wanted[owner : owner + 1, :]


def gather_kernel(block_count, incoming_ref, keys_ref, values_ref, out_ref):
    shards = incoming_ref.shape[0]
    head_size = out_ref.shape[2] // 2
    block_size = out_ref.shape[1] // CAP

    def owner_step(owner, carry):
        for slot in range(CAP):
            unit = jnp.maximum(incoming_ref[owner, 0, slot], 0)
            head = lax.div(unit, block_count)
            block = lax.rem(unit, block_count)
            rows = pl.ds(pl.multiple_of(block * block_size, block_size), block_size)
            lanes = pl.ds(pl.multiple_of(head * head_size, head_size), head_size)
            place = slice(slot * block_size, (slot + 1) * block_size)
            out_ref[owner, place, :head_size] = keys_ref[rows, lanes]
            out_ref[owner, place, head_size:] = values_ref[rows, lanes]
        return carry

    lax.fori_loop(0, shards, owner_step, 0, unroll=2)


def own_kernel(
    block_count,
    bits_ref,
    q_ref,
    k_ref,
    v_ref,
    o_ref,
    do_ref,
    lse_ref,
    dq_ref,
    dk_ref,
    dv_ref,
    delta_ref,
):
    tokens, head_size = q_ref.shape
    block_size = tokens // block_count
    scale = head_size ** (-0.5)
    head = pl.program_id(0)
    first = lax.axis_index("seq") * block_count
    q = q_ref[...]
    k = k_ref[...]
    v = v_ref[...]
    do = do_ref[...]
    product = do.astype(jnp.float32) * o_ref[...].astype(jnp.float32)
    ones = jnp.ones((8, head_size), jnp.float32)
    delta = dot_nt(ones, product, lax.Precision.HIGHEST)[:1]
    delta_ref[pl.ds(head, 1), :] = delta
    log_row = lse_ref[pl.ds(head, 1), :]
    lane_block = lax.div(lax.broadcasted_iota(jnp.int32, (1, tokens), 1), block_size)
    rows = []
    for block in range(block_count):
        bits = bits_ref[head, first + block]
        chosen = jnp.bitwise_and(jnp.right_shift(bits, lane_block), 1) == 1
        rows.append(
            jnp.broadcast_to(jnp.where(chosen, log_row, jnp.float32(FAR)), (block_size, tokens))
        )
    shift = jnp.concatenate(rows, axis=0)
    causal = lax.broadcasted_iota(jnp.int32, (tokens, tokens), 0) <= lax.broadcasted_iota(
        jnp.int32, (tokens, tokens), 1
    )
    scores = dot_nt(k, q) * scale
    probs = jnp.where(causal, jnp.exp(scores - shift), jnp.float32(0.0))
    dprobs = dot_nt(v, do)
    dscores = (probs * (dprobs - delta)).astype(jnp.bfloat16)
    dv_ref[...] = dot_nn(probs.astype(jnp.bfloat16), do)
    dk_ref[...] = dot_nn(dscores, q) * scale
    dq_ref[...] = dot_tn(dscores, k)


def pulled_kernel(
    block_count,
    wanted_ref,
    bits_ref,
    pulled_ref,
    q_ref,
    do_ref,
    lse_ref,
    delta_ref,
    own_dq_ref,
    far_ref,
    near_ref,
    grads_ref,
    dq_ref,
):
    tokens = q_ref.shape[0]
    head_size = pulled_ref.shape[2] // 2
    block_size = pulled_ref.shape[1] // CAP
    scale = head_size ** (-0.5)
    lane_block = lax.div(lax.broadcasted_iota(jnp.int32, (1, tokens), 1), block_size)
    dq_ref[...] = own_dq_ref[...]

    def owner_step(owner, carry):
        for slot in range(CAP):
            unit = wanted_ref[owner, 0, slot]
            safe = jnp.maximum(unit, 0)
            head = lax.div(safe, block_count)
            block = lax.rem(safe, block_count)
            bits = jnp.where(unit >= 0, bits_ref[head, owner * block_count + block], 0)
            lanes = pl.ds(pl.multiple_of(head * head_size, head_size), head_size)
            place = slice(slot * block_size, (slot + 1) * block_size)
            q = q_ref[:, lanes]
            do = do_ref[:, lanes]
            k = pulled_ref[owner, place, :head_size]
            v = pulled_ref[owner, place, head_size:]
            chosen = jnp.bitwise_and(jnp.right_shift(bits, lane_block), 1) == 1
            shift = jnp.where(chosen, lse_ref[pl.ds(head, 1), :], jnp.float32(FAR))
            probs = jnp.exp(dot_nt(k, q) * scale - shift)
            dprobs = dot_nt(v, do)
            dscores = (probs * (dprobs - delta_ref[pl.ds(head, 1), :])).astype(jnp.bfloat16)
            grads_ref[owner, place, :head_size] = (dot_nn(dscores, q) * scale).astype(
                grads_ref.dtype
            )
            grads_ref[owner, place, head_size:] = dot_nn(probs.astype(jnp.bfloat16), do).astype(
                grads_ref.dtype
            )
            dq_ref[:, lanes] += dot_tn(dscores, k)
        return carry

    lax.fori_loop(0, lax.axis_index("seq"), owner_step, 0)
    part = near_ref.shape[0] // 2
    here = lax.axis_index("head")
    for ref, offset, place in ((far_ref, 3, 0), (far_ref, 2, 1), (near_ref, 1, 0), (near_ref, 0, 1)):
        start = pl.multiple_of(jnp.bitwise_xor(here, offset) * part, part)
        ref[place * part : (place + 1) * part, :] = (dq_ref[pl.ds(start, part), :] * scale).astype(
            ref.dtype
        )


def finish_kernel(
    block_count, incoming_ref, returned_ref, own_dk_ref, own_dv_ref, dk_out, dv_out, dk_ref, dv_ref
):
    shards = incoming_ref.shape[0]
    head_size = returned_ref.shape[2] // 2
    block_size = returned_ref.shape[1] // CAP
    dk_ref[...] = own_dk_ref[...]
    dv_ref[...] = own_dv_ref[...]

    def owner_step(owner, carry):
        for slot in range(CAP):
            unit = incoming_ref[owner, 0, slot]

            @pl.when(unit >= 0)
            def _():
                head = lax.div(unit, block_count)
                block = lax.rem(unit, block_count)
                rows = pl.ds(pl.multiple_of(block * block_size, block_size), block_size)
                lanes = pl.ds(pl.multiple_of(head * head_size, head_size), head_size)
                place = slice(slot * block_size, (slot + 1) * block_size)
                dk_ref[rows, lanes] += returned_ref[owner, place, :head_size].astype(jnp.float32)
                dv_ref[rows, lanes] += returned_ref[owner, place, head_size:].astype(jnp.float32)

        return carry

    lax.fori_loop(lax.axis_index("seq") + 1, shards, owner_step, 0)
    dk_out[...] = dk_ref[...].astype(dk_out.dtype)
    dv_out[...] = dv_ref[...].astype(dv_out.dtype)


def per_device(queries, keys, values, outputs, out_grad, log_sum, selected, w_query):
    tokens, row_width = queries.shape
    head_count, block_count, pick_count = selected.shape
    head_size = row_width // head_count
    block_size = tokens // block_count
    shards = lax.axis_size("seq")
    groups = lax.axis_size("head")
    assert groups == 4
    width = pl.cdiv(shards * block_count, LANES) * LANES
    f32 = jnp.float32
    bf16 = jnp.bfloat16
    shape = jax.ShapeDtypeStruct

    def params(mib):
        return pltpu.CompilerParams(vmem_limit_bytes=mib << 20)

    def cost(flops, moved):
        return pl.CostEstimate(flops=flops, bytes_accessed=moved, transcendentals=0)

    wanted, bits = pl.pallas_call(
        functools.partial(index_kernel, shards),
        out_shape=(
            shape((shards, 1, LANES), jnp.int32),
            shape((head_count, width), jnp.int32),
        ),
        in_specs=[VMEM],
        out_specs=(VMEM, VMEM),
        compiler_params=params(4),
        name="index",
    )(selected)
    incoming = lax.all_to_all(wanted, "seq", split_axis=0, concat_axis=0, tiled=True)
    exchange = (shards, CAP * block_size, 2 * head_size)
    outgoing = pl.pallas_call(
        functools.partial(gather_kernel, block_count),
        out_shape=shape(exchange, bf16),
        in_specs=[SMEM, VMEM, VMEM],
        out_specs=VMEM,
        compiler_params=params(12),
        name="gather",
    )(incoming, keys, values)
    pulled = lax.all_to_all(outgoing, "seq", split_axis=0, concat_axis=0, tiled=True)

    column = pl.BlockSpec((tokens, head_size), lambda h: (0, h))
    whole = pl.BlockSpec((head_count, tokens), lambda h: (0, 0))
    unit_flops = 10 * tokens * block_size * head_size
    own_dq, own_dk, own_dv, delta = pl.pallas_call(
        functools.partial(own_kernel, block_count),
        grid=(head_count,),
        out_shape=(
            shape((tokens, row_width), f32),
            shape((tokens, row_width), f32),
            shape((tokens, row_width), f32),
            shape((head_count, tokens), f32),
        ),
        in_specs=[SMEM, column, column, column, column, column, whole],
        out_specs=(column, column, column, whole),
        compiler_params=params(12),
        cost_estimate=cost(
            8 * unit_flops * head_count * block_count, 22 * tokens * row_width
        ),
        name="own",
    )(bits, queries, keys, values, outputs, out_grad, log_sum)

    far, near, grads = pl.pallas_call(
        functools.partial(pulled_kernel, block_count),
        out_shape=(
            shape((tokens // 2, row_width), bf16),
            shape((tokens // 2, row_width), bf16),
            shape(exchange, bf16),
        ),
        in_specs=[SMEM, SMEM] + [VMEM] * 6,
        out_specs=(VMEM, VMEM, VMEM),
        scratch_shapes=[pltpu.VMEM((tokens, row_width), f32)],
        compiler_params=params(24),
        cost_estimate=cost(unit_flops * shards * CAP, 10 * tokens * row_width),
        name="pulled",
    )(wanted, bits, pulled, queries, out_grad, log_sum, delta, own_dq)

    returned = lax.all_to_all(grads, "seq", split_axis=0, concat_axis=0, tiled=True)
    key_gradient, value_gradient = pl.pallas_call(
        functools.partial(finish_kernel, block_count),
        out_shape=(shape((tokens, row_width), bf16), shape((tokens, row_width), bf16)),
        in_specs=[SMEM, VMEM, VMEM, VMEM],
        out_specs=(VMEM, VMEM),
        scratch_shapes=[pltpu.VMEM((tokens, row_width), f32)] * 2,
        compiler_params=params(16),
        name="finish",
    )(incoming, returned, own_dk, own_dv)

    part = tokens // groups
    beside = [(i, i ^ 1) for i in range(groups)]
    across = [(i, i ^ 2) for i in range(groups)]
    far_rows = dot_nt(far, w_query).astype(bf16)
    far_got = lax.ppermute(far_rows[:part], "head", beside)
    far_sum = (far_rows[part:].astype(f32) + far_got.astype(f32)).astype(bf16)
    across_got = lax.ppermute(far_sum, "head", across)
    near_rows = dot_nt(near, w_query)
    near_got = lax.ppermute(near_rows[:part].astype(bf16), "head", beside)
    x_grad = (near_rows[part:] + near_got.astype(f32) + across_got.astype(f32)).astype(bf16)
    return (x_grad, key_gradient, value_gradient)


def solution(mesh):
    return jax.shard_map(
        per_device,
        mesh=mesh,
        in_specs=(
            P("seq", "head"),
            P("seq", "head"),
            P("seq", "head"),
            P("seq", "head"),
            P("seq", "head"),
            P("head", "seq"),
            P("head", "seq", None),
            P(None, "head"),
        ),
        out_specs=(P(("seq", "head"), None), P("seq", "head"), P("seq", "head")),
        check_vma=False,
    )
```

```python
import functools

import jax
import jax.numpy as jnp
from jax import lax
from jax.experimental import pallas as pl
from jax.experimental.pallas import tpu as pltpu
from jax.sharding import PartitionSpec as P

CAP = 2
LANES = 128
FAR = 1e30
NONE = 1 << 20
VMEM_BYTES = 67043328
VMEM_SPARE = 256 << 10

VMEM = pl.BlockSpec(memory_space=pltpu.VMEM)
SMEM = pl.BlockSpec(memory_space=pltpu.SMEM)
HBM = pl.BlockSpec(memory_space=pltpu.HBM)


def dot_nt(a, b, precision=None):
    return lax.dot_general(
        a, b, (((1,), (1,)), ((), ())), preferred_element_type=jnp.float32, precision=precision
    )


def dot_nn(a, b):
    return lax.dot_general(a, b, (((1,), (0,)), ((), ())), preferred_element_type=jnp.float32)


def dot_tn(a, b):
    return lax.dot_general(a, b, (((0,), (0,)), ((), ())), preferred_element_type=jnp.float32)


def index_kernel(shards, selected_ref, wanted_ref, bits_ref):
    head_count, block_count, pick_count = selected_ref.shape
    width = bits_ref.shape[1]
    me = lax.axis_index("seq")
    lane = lax.broadcasted_iota(jnp.int32, (block_count, width), 1)
    weight = jnp.left_shift(1, lax.broadcasted_iota(jnp.int32, (block_count, width), 0))
    for head in range(head_count):
        rows = selected_ref[head]
        hits = jnp.zeros((block_count, width), jnp.int32)
        for pick in range(pick_count):
            hits = jnp.where(rows[:, pick : pick + 1] == lane, weight, hits)
        bits_ref[head : head + 1, :] = jnp.sum(hits, axis=0, keepdims=True)
    bits = bits_ref[...]
    lane = lax.broadcasted_iota(jnp.int32, (head_count, width), 1)
    label = lax.broadcasted_iota(jnp.int32, (head_count, width), 0) * block_count + lax.rem(
        lane, block_count
    )
    label = jnp.where((bits > 0) & (lax.div(lane, block_count) != me), label, NONE)
    owner_lane = lax.div(lax.broadcasted_iota(jnp.int32, (shards, width), 1), block_count)
    mine = owner_lane == lax.broadcasted_iota(jnp.int32, (shards, width), 0)
    column = lax.broadcasted_iota(jnp.int32, (shards, LANES), 1)
    wanted = jnp.full((shards, LANES), -1, jnp.int32)
    for slot in range(CAP):
        lowest = jnp.min(label, axis=0, keepdims=True)
        slot_value = jnp.min(jnp.where(mine, lowest, NONE), axis=1, keepdims=True)
        wanted = jnp.where((column == slot) & (slot_value < NONE), slot_value, wanted)
        taken = jnp.min(jnp.where(mine, slot_value, NONE), axis=0, keepdims=True)
        label = jnp.where(label == taken, NONE, label)
    for owner in range(shards):
        wanted_ref[owner] = wanted[owner : owner + 1, :]


def gather_kernel(block_count, incoming_ref, keys_ref, values_ref, out_ref, held_ref, in_sems, out_sems):
    shards = incoming_ref.shape[0]
    head_size = out_ref.shape[2] // 2
    block_size = out_ref.shape[1] // CAP

    def fetch(owner, carry):
        for slot in range(CAP):
            unit = jnp.maximum(incoming_ref[owner, 0, slot], 0)
            head = lax.div(unit, block_count)
            block = lax.rem(unit, block_count)
            rows = pl.ds(pl.multiple_of(block * block_size, block_size), block_size)
            lanes = pl.ds(pl.multiple_of(head * head_size, head_size), head_size)
            place = slice(slot * block_size, (slot + 1) * block_size)
            for ref, half in ((keys_ref, 0), (values_ref, 1)):
                pltpu.make_async_copy(
                    ref.at[rows, lanes],
                    held_ref.at[owner, place, half * head_size : (half + 1) * head_size],
                    in_sems.at[owner],
                ).start()
        return carry

    def forward(owner, carry):
        pltpu.make_async_copy(out_ref.at[owner], held_ref.at[owner], in_sems.at[owner]).wait()
        pltpu.make_async_copy(held_ref.at[owner], out_ref.at[owner], out_sems.at[owner]).start()
        return carry

    def drain(owner, carry):
        pltpu.make_async_copy(held_ref.at[owner], out_ref.at[owner], out_sems.at[owner]).wait()
        return carry

    lax.fori_loop(0, shards, fetch, 0)
    lax.fori_loop(0, shards, forward, 0)
    lax.fori_loop(0, shards, drain, 0)


def own_kernel(
    block_count,
    bits_ref,
    q_hbm,
    k_hbm,
    v_hbm,
    o_hbm,
    do_hbm,
    lse_hbm,
    dq_hbm,
    dk_hbm,
    dv_hbm,
    delta_ref,
    lse_ref,
    in_ref,
    out_ref,
    lse_sem,
    in_sems,
    out_sems,
):
    head_count, tokens = delta_ref.shape
    head_size = q_hbm.shape[1] // head_count
    block_size = tokens // block_count
    scale = head_size ** (-0.5)
    first = lax.axis_index("seq") * block_count

    def lanes(head):
        return pl.ds(pl.multiple_of(head * head_size, head_size), head_size)

    def load(head, at):
        source = (q_hbm, k_hbm, v_hbm, o_hbm, do_hbm)[at]
        return pltpu.make_async_copy(
            source.at[:, lanes(head)], in_ref.at[at, :, lanes(head)], in_sems.at[at, head]
        )

    def store(head, at):
        target = (dq_hbm, dk_hbm, dv_hbm)[at]
        return pltpu.make_async_copy(
            out_ref.at[at, :, lanes(head)], target.at[:, lanes(head)], out_sems.at[at, head]
        )

    load_lse = pltpu.make_async_copy(lse_hbm, lse_ref, lse_sem)
    load_lse.start()

    def begin(head, carry):
        for at in range(5):
            load(head, at).start()
        return carry

    lax.fori_loop(0, head_count, begin, 0)
    load_lse.wait()
    lane_block = lax.div(lax.broadcasted_iota(jnp.int32, (1, tokens), 1), block_size)
    causal = lax.broadcasted_iota(jnp.int32, (tokens, tokens), 0) <= lax.broadcasted_iota(
        jnp.int32, (tokens, tokens), 1
    )
    ones = jnp.ones((8, head_size), jnp.float32)

    def head_step(head, carry):
        for at in range(5):
            load(head, at).wait()
        q, k, v, o, do = (in_ref[at, :, lanes(head)] for at in range(5))
        product = do.astype(jnp.float32) * o.astype(jnp.float32)
        delta = dot_nt(ones, product, lax.Precision.HIGHEST)[:1]
        delta_ref[pl.ds(head, 1), :] = delta
        log_row = lse_ref[pl.ds(head, 1), :]
        rows = []
        for block in range(block_count):
            bits = bits_ref[head, first + block]
            chosen = jnp.bitwise_and(jnp.right_shift(bits, lane_block), 1) == 1
            rows.append(
                jnp.broadcast_to(jnp.where(chosen, log_row, jnp.float32(FAR)), (block_size, tokens))
            )
        shift = jnp.concatenate(rows, axis=0)
        scores = dot_nt(k, q) * scale
        probs = jnp.where(causal, jnp.exp(scores - shift), jnp.float32(0.0))
        dprobs = dot_nt(v, do)
        dscores = (probs * (dprobs - delta)).astype(jnp.bfloat16)
        out_ref[2, :, lanes(head)] = dot_nn(probs.astype(jnp.bfloat16), do)
        out_ref[1, :, lanes(head)] = dot_nn(dscores, q) * scale
        out_ref[0, :, lanes(head)] = dot_tn(dscores, k)
        for at in range(3):
            store(head, at).start()
        return carry

    lax.fori_loop(0, head_count, head_step, 0)

    def end(head, carry):
        for at in range(3):
            store(head, at).wait()
        return carry

    lax.fori_loop(0, head_count, end, 0)


def pulled_kernel(
    block_count,
    wanted_ref,
    bits_ref,
    pulled_hbm,
    q_hbm,
    do_hbm,
    lse_hbm,
    delta_hbm,
    own_dq_hbm,
    w_hbm,
    send_ref,
    keep_ref,
    near_ref,
    grads_hbm,
    pulled_ref,
    q_ref,
    do_ref,
    lse_ref,
    delta_ref,
    dq_ref,
    w_ref,
    grads_ref,
    rows_ref,
    in_sems,
    w_sems,
    out_sem,
):
    tokens = q_ref.shape[0]
    head_size = pulled_ref.shape[2] // 2
    block_size = pulled_ref.shape[1] // CAP
    scale = head_size ** (-0.5)
    loads = [
        pltpu.make_async_copy(source, target, in_sems.at[at])
        for at, (source, target) in enumerate(
            (
                (q_hbm, q_ref),
                (do_hbm, do_ref),
                (pulled_hbm, pulled_ref),
                (lse_hbm, lse_ref),
                (delta_hbm, delta_ref),
                (own_dq_hbm, dq_ref),
            )
        )
    ]
    chunks = w_sems.shape[0]
    chunk = w_ref.shape[0] // chunks

    def load_w(at):
        rows = pl.ds(pl.multiple_of(at * chunk, chunk), chunk)
        return pltpu.make_async_copy(w_hbm.at[rows], w_ref.at[rows], w_sems.at[at])

    for load in loads:
        load.start()
    for at in range(chunks):
        load_w(at).start()
    for load in loads:
        load.wait()
    lane_block = lax.div(lax.broadcasted_iota(jnp.int32, (1, tokens), 1), block_size)

    def owner_step(step, carry):
        sums = []
        for owner in (step * 2, step * 2 + 1):
            for slot in range(CAP):
                unit = wanted_ref[owner, 0, slot]
                safe = jnp.maximum(unit, 0)
                head = lax.div(safe, block_count)
                block = lax.rem(safe, block_count)
                bits = jnp.where(unit >= 0, bits_ref[head, owner * block_count + block], 0)
                lanes = pl.ds(pl.multiple_of(head * head_size, head_size), head_size)
                place = slice(slot * block_size, (slot + 1) * block_size)
                q = q_ref[:, lanes]
                do = do_ref[:, lanes]
                k = pulled_ref[owner, place, :head_size]
                v = pulled_ref[owner, place, head_size:]
                chosen = jnp.bitwise_and(jnp.right_shift(bits, lane_block), 1) == 1
                shift = jnp.where(chosen, lse_ref[pl.ds(head, 1), :], jnp.float32(FAR))
                probs = jnp.exp(dot_nt(k, q) * scale - shift)
                dprobs = dot_nt(v, do)
                dscores = (probs * (dprobs - delta_ref[pl.ds(head, 1), :])).astype(jnp.bfloat16)
                grads_ref[owner, place, :head_size] = (dot_nn(dscores, q) * scale).astype(
                    grads_ref.dtype
                )
                grads_ref[owner, place, head_size:] = dot_nn(
                    probs.astype(jnp.bfloat16), do
                ).astype(grads_ref.dtype)
                sums.append((lanes, dot_tn(dscores, k)))
        for lanes, value in sums:
            dq_ref[:, lanes] += value
        return carry

    lax.fori_loop(0, lax.div(lax.axis_index("seq") + 1, 2), owner_step, 0)
    store = pltpu.make_async_copy(grads_ref, grads_hbm, out_sem)
    store.start()
    part = near_ref.shape[0] // 2
    here = lax.axis_index("head")
    for ref, offset, place in (
        (rows_ref, 3, 0),
        (rows_ref, 2, 1),
        (near_ref, 1, 0),
        (near_ref, 0, 1),
    ):
        start = pl.multiple_of(jnp.bitwise_xor(here, offset) * part, part)
        ref[place * part : (place + 1) * part, :] = (dq_ref[pl.ds(start, part), :] * scale).astype(
            ref.dtype
        )
    for at in range(chunks):
        load_w(at).wait()
        columns = slice(at * chunk, (at + 1) * chunk)
        product = dot_nt(rows_ref[...], w_ref[columns, :]).astype(send_ref.dtype)
        send_ref[:, columns] = product[:part]
        keep_ref[:, columns] = product[part:]
    store.wait()


def near_kernel(rows_ref, w_ref, send_ref, keep_ref):
    part = send_ref.shape[0]
    product = dot_nt(rows_ref[...], w_ref[...])
    send_ref[...] = product[:part].astype(send_ref.dtype)
    keep_ref[...] = product[part:].astype(keep_ref.dtype)


def finish_kernel(
    block_count,
    incoming_ref,
    returned_hbm,
    own_dk_hbm,
    own_dv_hbm,
    dk_out,
    dv_out,
    returned_ref,
    dk_ref,
    dv_ref,
    sems,
):
    shards = incoming_ref.shape[0]
    head_size = returned_ref.shape[2] // 2
    block_size = returned_ref.shape[1] // CAP
    loads = [
        pltpu.make_async_copy(source, target, sems.at[at])
        for at, (source, target) in enumerate(
            ((returned_hbm, returned_ref), (own_dk_hbm, dk_ref), (own_dv_hbm, dv_ref))
        )
    ]
    for load in loads:
        load.start()
    for load in loads:
        load.wait()

    def owner_step(owner, carry):
        for slot in range(CAP):
            unit = incoming_ref[owner, 0, slot]

            @pl.when(unit >= 0)
            def _():
                head = lax.div(unit, block_count)
                block = lax.rem(unit, block_count)
                rows = pl.ds(pl.multiple_of(block * block_size, block_size), block_size)
                lanes = pl.ds(pl.multiple_of(head * head_size, head_size), head_size)
                place = slice(slot * block_size, (slot + 1) * block_size)
                dk_ref[rows, lanes] += returned_ref[owner, place, :head_size].astype(jnp.float32)
                dv_ref[rows, lanes] += returned_ref[owner, place, head_size:].astype(jnp.float32)

        return carry

    lax.fori_loop(lax.axis_index("seq") + 1, shards, owner_step, 0)
    dk_out[...] = dk_ref[...].astype(dk_out.dtype)
    dv_out[...] = dv_ref[...].astype(dv_out.dtype)


def per_device(queries, keys, values, outputs, out_grad, log_sum, selected, w_query):
    tokens, row_width = queries.shape
    head_count, block_count, pick_count = selected.shape
    head_size = row_width // head_count
    block_size = tokens // block_count
    shards = lax.axis_size("seq")
    groups = lax.axis_size("head")
    assert groups == 4
    width = pl.cdiv(shards * block_count, LANES) * LANES
    f32 = jnp.float32
    bf16 = jnp.bfloat16
    shape = jax.ShapeDtypeStruct

    def params(spare=VMEM_SPARE):
        return pltpu.CompilerParams(vmem_limit_bytes=VMEM_BYTES - spare)

    def cost(flops, moved):
        return pl.CostEstimate(flops=flops, bytes_accessed=moved, transcendentals=0)

    wanted, bits = pl.pallas_call(
        functools.partial(index_kernel, shards),
        out_shape=(
            shape((shards, 1, LANES), jnp.int32),
            shape((head_count, width), jnp.int32),
        ),
        in_specs=[VMEM],
        out_specs=(VMEM, VMEM),
        compiler_params=params(),
        name="index",
    )(selected)
    incoming = lax.all_to_all(wanted, "seq", split_axis=0, concat_axis=0, tiled=True)
    exchange = (shards, CAP * block_size, 2 * head_size)
    outgoing = pl.pallas_call(
        functools.partial(gather_kernel, block_count),
        out_shape=shape(exchange, bf16),
        in_specs=[SMEM, HBM, HBM],
        out_specs=HBM,
        scratch_shapes=[
            pltpu.VMEM(exchange, bf16),
            pltpu.SemaphoreType.DMA((shards,)),
            pltpu.SemaphoreType.DMA((shards,)),
        ],
        compiler_params=params(),
        name="gather",
    )(incoming, keys, values)
    pulled = lax.all_to_all(outgoing, "seq", split_axis=0, concat_axis=0, tiled=True)

    unit_flops = 10 * tokens * block_size * head_size
    own_dq, own_dk, own_dv, delta = pl.pallas_call(
        functools.partial(own_kernel, block_count),
        out_shape=(
            shape((tokens, row_width), f32),
            shape((tokens, row_width), f32),
            shape((tokens, row_width), f32),
            shape((head_count, tokens), f32),
        ),
        in_specs=[SMEM] + [HBM] * 6,
        out_specs=(HBM, HBM, HBM, VMEM),
        scratch_shapes=[
            pltpu.VMEM((head_count, tokens), f32),
            pltpu.VMEM((5, tokens, row_width), bf16),
            pltpu.VMEM((3, tokens, row_width), f32),
            pltpu.SemaphoreType.DMA,
            pltpu.SemaphoreType.DMA((5, head_count)),
            pltpu.SemaphoreType.DMA((3, head_count)),
        ],
        compiler_params=params(),
        cost_estimate=cost(8 * unit_flops * head_count * block_count, 22 * tokens * row_width),
        name="own",
    )(bits, queries, keys, values, outputs, out_grad, log_sum)

    part = tokens // groups
    features = w_query.shape[0]
    chunks = 8
    far_send, far_keep, near, grads = pl.pallas_call(
        functools.partial(pulled_kernel, block_count),
        out_shape=(
            shape((part, features), bf16),
            shape((part, features), bf16),
            shape((2 * part, row_width), bf16),
            shape(exchange, bf16),
        ),
        in_specs=[SMEM, SMEM] + [HBM] * 7,
        out_specs=(VMEM, VMEM, VMEM, HBM),
        scratch_shapes=[
            pltpu.VMEM(exchange, bf16),
            pltpu.VMEM((tokens, row_width), bf16),
            pltpu.VMEM((tokens, row_width), bf16),
            pltpu.VMEM((head_count, tokens), f32),
            pltpu.VMEM((head_count, tokens), f32),
            pltpu.VMEM((tokens, row_width), f32),
            pltpu.VMEM(w_query.shape, bf16),
            pltpu.VMEM(exchange, bf16),
            pltpu.VMEM((2 * part, row_width), bf16),
            pltpu.SemaphoreType.DMA((6,)),
            pltpu.SemaphoreType.DMA((chunks,)),
            pltpu.SemaphoreType.DMA,
        ],
        compiler_params=params(),
        cost_estimate=cost(unit_flops * shards * CAP, 10 * tokens * row_width),
        name="pulled",
    )(wanted, bits, pulled, queries, out_grad, log_sum, delta, own_dq, w_query)

    beside = [(i, i ^ 1) for i in range(groups)]
    across = [(i, i ^ 2) for i in range(groups)]
    far_got = lax.ppermute(far_send, "head", beside)
    far_sum = (far_keep.astype(f32) + far_got.astype(f32)).astype(bf16)
    across_got = lax.ppermute(far_sum, "head", across)

    near_send, near_keep = pl.pallas_call(
        near_kernel,
        grid=(chunks,),
        out_shape=(shape((part, features), bf16), shape((part, features), f32)),
        in_specs=[
            pl.BlockSpec((2 * part, row_width), lambda i: (0, 0)),
            pl.BlockSpec((features // chunks, row_width), lambda i: (i, 0)),
        ],
        out_specs=(
            pl.BlockSpec((part, features // chunks), lambda i: (0, i)),
            pl.BlockSpec((part, features // chunks), lambda i: (0, i)),
        ),
        compiler_params=params(),
        cost_estimate=cost(4 * part * row_width * features, 2 * row_width * features),
        name="near",
    )(near, w_query)
    near_got = lax.ppermute(near_send, "head", beside)
    near_sum = lax.optimization_barrier(near_keep + near_got.astype(f32))

    returned = lax.all_to_all(grads, "seq", split_axis=0, concat_axis=0, tiled=True)
    key_gradient, value_gradient = pl.pallas_call(
        functools.partial(finish_kernel, block_count),
        out_shape=(shape((tokens, row_width), bf16), shape((tokens, row_width), bf16)),
        in_specs=[SMEM, HBM, HBM, HBM],
        out_specs=(VMEM, VMEM),
        scratch_shapes=[
            pltpu.VMEM(exchange, bf16),
            pltpu.VMEM((tokens, row_width), f32),
            pltpu.VMEM((tokens, row_width), f32),
            pltpu.SemaphoreType.DMA((3,)),
        ],
        compiler_params=params(),
        name="finish",
    )(incoming, returned, own_dk, own_dv)
    x_grad = (near_sum + across_got.astype(f32)).astype(bf16)
    return (x_grad, key_gradient, value_gradient)


def solution(mesh):
    return jax.shard_map(
        per_device,
        mesh=mesh,
        in_specs=(
            P("seq", "head"),
            P("seq", "head"),
            P("seq", "head"),
            P("seq", "head"),
            P("seq", "head"),
            P("head", "seq"),
            P("head", "seq", None),
            P(None, "head"),
        ),
        out_specs=(P(("seq", "head"), None), P("seq", "head"), P("seq", "head")),
        check_vma=False,
    )
```

```python
import functools

import jax
import jax.numpy as jnp
from jax import lax
from jax.experimental import pallas as pl
from jax.experimental.pallas import tpu as pltpu
from jax.sharding import PartitionSpec as P

CAP = 2
LANES = 128
FAR = 1e30
NONE = 1 << 20
VMEM_BYTES = 67043328
VMEM_SPARE = 40 << 20

VMEM = pl.BlockSpec(memory_space=pltpu.VMEM)
SMEM = pl.BlockSpec(memory_space=pltpu.SMEM)
HBM = pl.BlockSpec(memory_space=pltpu.HBM)


def dot_nt(a, b, precision=None):
    return lax.dot_general(
        a, b, (((1,), (1,)), ((), ())), preferred_element_type=jnp.float32, precision=precision
    )


def dot_nn(a, b):
    return lax.dot_general(a, b, (((1,), (0,)), ((), ())), preferred_element_type=jnp.float32)


def dot_tn(a, b):
    return lax.dot_general(a, b, (((0,), (0,)), ((), ())), preferred_element_type=jnp.float32)


def index_kernel(shards, selected_ref, wanted_ref, bits_ref):
    head_count, block_count, pick_count = selected_ref.shape
    width = bits_ref.shape[1]
    me = lax.axis_index("seq")
    lane = lax.broadcasted_iota(jnp.int32, (block_count, width), 1)
    weight = jnp.left_shift(1, lax.broadcasted_iota(jnp.int32, (block_count, width), 0))
    for head in range(head_count):
        rows = selected_ref[head]
        hits = jnp.zeros((block_count, width), jnp.int32)
        for pick in range(pick_count):
            hits = jnp.where(rows[:, pick : pick + 1] == lane, weight, hits)
        bits_ref[head : head + 1, :] = jnp.sum(hits, axis=0, keepdims=True)
    bits = bits_ref[...]
    lane = lax.broadcasted_iota(jnp.int32, (head_count, width), 1)
    label = lax.broadcasted_iota(jnp.int32, (head_count, width), 0) * block_count + lax.rem(
        lane, block_count
    )
    label = jnp.where((bits > 0) & (lax.div(lane, block_count) != me), label, NONE)
    owner_lane = lax.div(lax.broadcasted_iota(jnp.int32, (shards, width), 1), block_count)
    mine = owner_lane == lax.broadcasted_iota(jnp.int32, (shards, width), 0)
    column = lax.broadcasted_iota(jnp.int32, (shards, LANES), 1)
    wanted = jnp.full((shards, LANES), -1, jnp.int32)
    for slot in range(CAP):
        lowest = jnp.min(label, axis=0, keepdims=True)
        slot_value = jnp.min(jnp.where(mine, lowest, NONE), axis=1, keepdims=True)
        wanted = jnp.where((column == slot) & (slot_value < NONE), slot_value, wanted)
        taken = jnp.min(jnp.where(mine, slot_value, NONE), axis=0, keepdims=True)
        label = jnp.where(label == taken, NONE, label)
    for owner in range(shards):
        wanted_ref[owner] = wanted[owner : owner + 1, :]


def gather_kernel(block_count, incoming_ref, keys_ref, values_ref, out_ref, held_ref, in_sems, out_sems):
    shards = incoming_ref.shape[0]
    head_size = out_ref.shape[2] // 2
    block_size = out_ref.shape[1] // CAP

    def fetch(owner, carry):
        for slot in range(CAP):
            unit = jnp.maximum(incoming_ref[owner, 0, slot], 0)
            head = lax.div(unit, block_count)
            block = lax.rem(unit, block_count)
            rows = pl.ds(pl.multiple_of(block * block_size, block_size), block_size)
            lanes = pl.ds(pl.multiple_of(head * head_size, head_size), head_size)
            place = slice(slot * block_size, (slot + 1) * block_size)
            for ref, half in ((keys_ref, 0), (values_ref, 1)):
                pltpu.make_async_copy(
                    ref.at[rows, lanes],
                    held_ref.at[owner, place, half * head_size : (half + 1) * head_size],
                    in_sems.at[owner],
                ).start()
        return carry

    def forward(owner, carry):
        pltpu.make_async_copy(out_ref.at[owner], held_ref.at[owner], in_sems.at[owner]).wait()
        pltpu.make_async_copy(held_ref.at[owner], out_ref.at[owner], out_sems.at[owner]).start()
        return carry

    def drain(owner, carry):
        pltpu.make_async_copy(held_ref.at[owner], out_ref.at[owner], out_sems.at[owner]).wait()
        return carry

    lax.fori_loop(0, shards, fetch, 0)
    lax.fori_loop(0, shards, forward, 0)
    lax.fori_loop(0, shards, drain, 0)


def own_kernel(
    block_count,
    bits_ref,
    q_hbm,
    k_hbm,
    v_hbm,
    o_hbm,
    do_hbm,
    lse_hbm,
    q_ref,
    do_ref,
    lse_ref,
    delta_ref,
    dq_ref,
    dk_hbm,
    dv_hbm,
    k_ref,
    v_ref,
    o_ref,
    dk_ref,
    dv_ref,
    lse_sem,
    in_sems,
    out_sems,
):
    head_count, tokens = delta_ref.shape
    head_size = q_hbm.shape[1] // head_count
    block_size = tokens // block_count
    scale = head_size ** (-0.5)
    first = lax.axis_index("seq") * block_count
    pairs = ((q_hbm, q_ref), (k_hbm, k_ref), (v_hbm, v_ref), (o_hbm, o_ref), (do_hbm, do_ref))

    def columns(head):
        return pl.ds(pl.multiple_of(head * head_size, head_size), head_size)

    def load(head, at):
        source, target = pairs[at]
        lanes = columns(head)
        return pltpu.make_async_copy(
            source.at[:, lanes], target.at[:, lanes], in_sems.at[at, head]
        )

    load_lse = pltpu.make_async_copy(lse_hbm, lse_ref, lse_sem)
    load_lse.start()

    def begin(head, carry):
        for at in range(5):
            load(head, at).start()
        return carry

    lax.fori_loop(0, head_count, begin, 0)
    load_lse.wait()
    lane_block = lax.div(lax.broadcasted_iota(jnp.int32, (1, tokens), 1), block_size)
    causal = lax.broadcasted_iota(jnp.int32, (tokens, tokens), 0) <= lax.broadcasted_iota(
        jnp.int32, (tokens, tokens), 1
    )
    ones = jnp.ones((8, head_size), jnp.float32)

    def head_step(head, carry):
        for at in range(5):
            load(head, at).wait()
        lanes = columns(head)
        q, k, v, o, do = (ref[:, lanes] for ref in (q_ref, k_ref, v_ref, o_ref, do_ref))
        product = do.astype(jnp.float32) * o.astype(jnp.float32)
        delta = dot_nt(ones, product, lax.Precision.HIGHEST)[:1]
        delta_ref[pl.ds(head, 1), :] = delta
        log_row = lse_ref[pl.ds(head, 1), :]
        rows = []
        for block in range(block_count):
            bits = bits_ref[head, first + block]
            chosen = jnp.bitwise_and(jnp.right_shift(bits, lane_block), 1) == 1
            rows.append(
                jnp.broadcast_to(jnp.where(chosen, log_row, jnp.float32(FAR)), (block_size, tokens))
            )
        shift = jnp.concatenate(rows, axis=0)
        scores = dot_nt(k, q) * scale
        probs = jnp.where(causal, jnp.exp(scores - shift), jnp.float32(0.0))
        dprobs = dot_nt(v, do)
        dscores = (probs * (dprobs - delta)).astype(jnp.bfloat16)
        dv_ref[:, lanes] = dot_nn(probs.astype(jnp.bfloat16), do)
        dk_ref[:, lanes] = dot_nn(dscores, q) * scale
        dq_ref[:, lanes] = dot_tn(dscores, k)
        return carry

    lax.fori_loop(0, head_count, head_step, 0)
    stores = (
        pltpu.make_async_copy(dk_ref, dk_hbm, out_sems.at[0]),
        pltpu.make_async_copy(dv_ref, dv_hbm, out_sems.at[1]),
    )
    for store in stores:
        store.start()
    for store in stores:
        store.wait()


def pulled_kernel(
    block_count,
    wanted_ref,
    bits_ref,
    pulled_ref,
    q_ref,
    do_ref,
    lse_ref,
    delta_ref,
    own_dq_ref,
    w_hbm,
    far_send_ref,
    far_keep_ref,
    near_send_hbm,
    near_keep_hbm,
    grads_hbm,
    dq_ref,
    rows_ref,
    grads_ref,
    w_ref,
    near_send_ref,
    near_keep_ref,
    out_sem,
    w_sems,
    near_sems,
):
    chunks = w_sems.shape[0]
    chunk = w_ref.shape[0] // chunks

    def load_w(at):
        return pltpu.make_async_copy(
            w_hbm.at[pl.ds(at * chunk, chunk)], w_ref.at[pl.ds(at * chunk, chunk)], w_sems.at[at]
        )

    def store_near(at):
        columns = pl.ds(at * chunk, chunk)
        return [
            pltpu.make_async_copy(ref.at[:, columns], out.at[:, columns], near_sems.at[side, at])
            for side, (ref, out) in enumerate(
                ((near_send_ref, near_send_hbm), (near_keep_ref, near_keep_hbm))
            )
        ]

    for at in range(chunks):
        load_w(at).start()
    tokens = q_ref.shape[0]
    head_size = pulled_ref.shape[2] // 2
    block_size = pulled_ref.shape[1] // CAP
    scale = head_size ** (-0.5)
    lane_block = lax.div(lax.broadcasted_iota(jnp.int32, (1, tokens), 1), block_size)
    dq_ref[...] = own_dq_ref[...]

    def owner_step(step, carry):
        sums = []
        for owner in (step * 2, step * 2 + 1):
            for slot in range(CAP):
                unit = wanted_ref[owner, 0, slot]
                safe = jnp.maximum(unit, 0)
                head = lax.div(safe, block_count)
                block = lax.rem(safe, block_count)
                bits = jnp.where(unit >= 0, bits_ref[head, owner * block_count + block], 0)
                lanes = pl.ds(pl.multiple_of(head * head_size, head_size), head_size)
                place = slice(slot * block_size, (slot + 1) * block_size)
                q = q_ref[:, lanes]
                do = do_ref[:, lanes]
                k = pulled_ref[owner, place, :head_size]
                v = pulled_ref[owner, place, head_size:]
                chosen = jnp.bitwise_and(jnp.right_shift(bits, lane_block), 1) == 1
                shift = jnp.where(chosen, lse_ref[pl.ds(head, 1), :], jnp.float32(FAR))
                probs = jnp.exp(dot_nt(k, q) * scale - shift)
                dprobs = dot_nt(v, do)
                dscores = (probs * (dprobs - delta_ref[pl.ds(head, 1), :])).astype(jnp.bfloat16)
                grads_ref[owner, place, :head_size] = (dot_nn(dscores, q) * scale).astype(
                    grads_ref.dtype
                )
                grads_ref[owner, place, head_size:] = dot_nn(
                    probs.astype(jnp.bfloat16), do
                ).astype(grads_ref.dtype)
                sums.append((lanes, dot_tn(dscores, k)))
        for lanes, value in sums:
            dq_ref[:, lanes] += value
        return carry

    lax.fori_loop(0, lax.div(lax.axis_index("seq") + 1, 2), owner_step, 0)
    store = pltpu.make_async_copy(grads_ref, grads_hbm, out_sem)
    store.start()
    targets = (far_send_ref, far_keep_ref, near_send_ref, near_keep_ref)
    part = far_send_ref.shape[0]
    here = lax.axis_index("head")
    for place in range(4):
        start = pl.multiple_of(jnp.bitwise_xor(here, 3 - place) * part, part)
        rows_ref[place * part : (place + 1) * part, :] = (
            dq_ref[pl.ds(start, part), :] * scale
        ).astype(rows_ref.dtype)
    for at in range(chunks):
        load_w(at).wait()
        columns = slice(at * chunk, (at + 1) * chunk)
        product = dot_nt(rows_ref[...], w_ref[columns, :])
        for place, ref in enumerate(targets):
            ref[:, columns] = product[place * part : (place + 1) * part].astype(ref.dtype)
        for copy in store_near(at):
            copy.start()
    for at in range(chunks):
        for copy in store_near(at):
            copy.wait()
    store.wait()


def finish_kernel(
    block_count,
    incoming_ref,
    returned_ref,
    own_dk_hbm,
    own_dv_hbm,
    dk_out,
    dv_out,
    dk_ref,
    dv_ref,
    sems,
):
    shards = incoming_ref.shape[0]
    head_size = returned_ref.shape[2] // 2
    block_size = returned_ref.shape[1] // CAP
    loads = [
        pltpu.make_async_copy(source, target, sems.at[at])
        for at, (source, target) in enumerate(
            ((own_dk_hbm, dk_ref), (own_dv_hbm, dv_ref))
        )
    ]
    for load in loads:
        load.start()
    for load in loads:
        load.wait()

    def owner_step(owner, carry):
        for slot in range(CAP):
            unit = incoming_ref[owner, 0, slot]

            @pl.when(unit >= 0)
            def _():
                head = lax.div(unit, block_count)
                block = lax.rem(unit, block_count)
                rows = pl.ds(pl.multiple_of(block * block_size, block_size), block_size)
                lanes = pl.ds(pl.multiple_of(head * head_size, head_size), head_size)
                place = slice(slot * block_size, (slot + 1) * block_size)
                dk_ref[rows, lanes] += returned_ref[owner, place, :head_size].astype(jnp.float32)
                dv_ref[rows, lanes] += returned_ref[owner, place, head_size:].astype(jnp.float32)

        return carry

    lax.fori_loop(lax.axis_index("seq") + 1, shards, owner_step, 0)
    dk_out[...] = dk_ref[...].astype(dk_out.dtype)
    dv_out[...] = dv_ref[...].astype(dv_out.dtype)


def per_device(queries, keys, values, outputs, out_grad, log_sum, selected, w_query):
    tokens, row_width = queries.shape
    head_count, block_count, pick_count = selected.shape
    head_size = row_width // head_count
    block_size = tokens // block_count
    shards = lax.axis_size("seq")
    groups = lax.axis_size("head")
    assert groups == 4
    width = pl.cdiv(shards * block_count, LANES) * LANES
    queries, keys, values, outputs, out_grad, log_sum, w_query = (
        pltpu.with_memory_space_constraint(a, pltpu.HBM)
        for a in (queries, keys, values, outputs, out_grad, log_sum, w_query)
    )
    f32 = jnp.float32
    bf16 = jnp.bfloat16
    shape = jax.ShapeDtypeStruct

    def params(spare=VMEM_SPARE):
        return pltpu.CompilerParams(vmem_limit_bytes=VMEM_BYTES - spare)

    def cost(flops, moved):
        return pl.CostEstimate(flops=flops, bytes_accessed=moved, transcendentals=0)

    wanted, bits = pl.pallas_call(
        functools.partial(index_kernel, shards),
        out_shape=(
            shape((shards, 1, LANES), jnp.int32),
            shape((head_count, width), jnp.int32),
        ),
        in_specs=[VMEM],
        out_specs=(VMEM, VMEM),
        compiler_params=params(),
        name="index",
    )(selected)
    incoming = lax.all_to_all(wanted, "seq", split_axis=0, concat_axis=0, tiled=True)
    exchange = (shards, CAP * block_size, 2 * head_size)
    outgoing = pl.pallas_call(
        functools.partial(gather_kernel, block_count),
        out_shape=shape(exchange, bf16),
        in_specs=[SMEM, HBM, HBM],
        out_specs=HBM,
        scratch_shapes=[
            pltpu.VMEM(exchange, bf16),
            pltpu.SemaphoreType.DMA((shards,)),
            pltpu.SemaphoreType.DMA((shards,)),
        ],
        compiler_params=params(),
        name="gather",
    )(incoming, keys, values)
    pulled = lax.all_to_all(outgoing, "seq", split_axis=0, concat_axis=0, tiled=True)

    unit_flops = 10 * tokens * block_size * head_size
    q_here, do_here, lse_here, delta, own_dq, own_dk, own_dv = pl.pallas_call(
        functools.partial(own_kernel, block_count),
        out_shape=(
            shape((tokens, row_width), bf16),
            shape((tokens, row_width), bf16),
            shape((head_count, tokens), f32),
            shape((head_count, tokens), f32),
            shape((tokens, row_width), f32),
            pltpu.HBM((tokens, row_width), f32),
            pltpu.HBM((tokens, row_width), f32),
        ),
        in_specs=[SMEM] + [HBM] * 6,
        out_specs=(VMEM,) * 5 + (HBM, HBM),
        scratch_shapes=[
            pltpu.VMEM((tokens, row_width), bf16),
            pltpu.VMEM((tokens, row_width), bf16),
            pltpu.VMEM((tokens, row_width), bf16),
            pltpu.VMEM((tokens, row_width), f32),
            pltpu.VMEM((tokens, row_width), f32),
            pltpu.SemaphoreType.DMA,
            pltpu.SemaphoreType.DMA((5, head_count)),
            pltpu.SemaphoreType.DMA((2,)),
        ],
        compiler_params=params(),
        cost_estimate=cost(8 * unit_flops * head_count * block_count, 22 * tokens * row_width),
        name="own",
    )(bits, queries, keys, values, outputs, out_grad, log_sum)

    part = tokens // groups
    features = w_query.shape[0]
    far_send, far_keep, near_send, near_keep, grads = pl.pallas_call(
        functools.partial(pulled_kernel, block_count),
        out_shape=(
            shape((part, features), bf16),
            shape((part, features), bf16),
            pltpu.HBM((part, features), bf16),
            pltpu.HBM((part, features), bf16),
            pltpu.HBM(exchange, bf16),
        ),
        in_specs=[SMEM, SMEM] + [VMEM] * 6 + [HBM],
        out_specs=(VMEM, VMEM, HBM, HBM, HBM),
        scratch_shapes=[
            pltpu.VMEM((tokens, row_width), f32),
            pltpu.VMEM((tokens, row_width), bf16),
            pltpu.VMEM(exchange, bf16),
            pltpu.VMEM(w_query.shape, bf16),
            pltpu.VMEM((part, features), bf16),
            pltpu.VMEM((part, features), bf16),
            pltpu.SemaphoreType.DMA,
            pltpu.SemaphoreType.DMA((8,)),
            pltpu.SemaphoreType.DMA((2, 8)),
        ],
        compiler_params=params(),
        cost_estimate=cost(unit_flops * shards * CAP, 10 * tokens * row_width),
        name="pulled",
    )(wanted, bits, pulled, q_here, do_here, lse_here, delta, own_dq, w_query)

    beside = [(i, i ^ 1) for i in range(groups)]
    across = [(i, i ^ 2) for i in range(groups)]
    far_got = lax.ppermute(far_send, "head", beside)
    far_sum = (far_keep.astype(f32) + far_got.astype(f32)).astype(bf16)
    across_got = lax.ppermute(far_sum, "head", across)

    near_got = lax.ppermute(near_send, "head", beside)
    returned = lax.all_to_all(grads, "seq", split_axis=0, concat_axis=0, tiled=True)
    own_dk, own_dv = (
        pltpu.with_memory_space_constraint(a, pltpu.HBM) for a in (own_dk, own_dv)
    )
    key_gradient, value_gradient = pl.pallas_call(
        functools.partial(finish_kernel, block_count),
        out_shape=(shape((tokens, row_width), bf16), shape((tokens, row_width), bf16)),
        in_specs=[SMEM, VMEM, HBM, HBM],
        out_specs=(VMEM, VMEM),
        scratch_shapes=[
            pltpu.VMEM((tokens, row_width), f32),
            pltpu.VMEM((tokens, row_width), f32),
            pltpu.SemaphoreType.DMA((2,)),
        ],
        compiler_params=params(),
        name="finish",
    )(incoming, returned, own_dk, own_dv)
    x_grad = (near_keep.astype(f32) + near_got.astype(f32) + across_got.astype(f32)).astype(bf16)
    return (x_grad, key_gradient, value_gradient)


def solution(mesh):
    return jax.shard_map(
        per_device,
        mesh=mesh,
        in_specs=(
            P("seq", "head"),
            P("seq", "head"),
            P("seq", "head"),
            P("seq", "head"),
            P("seq", "head"),
            P("head", "seq"),
            P("head", "seq", None),
            P(None, "head"),
        ),
        out_specs=(P(("seq", "head"), None), P("seq", "head"), P("seq", "head")),
        check_vma=False,
    )
```

```python
import functools

import jax
import jax.numpy as jnp
from jax import lax
from jax.experimental import pallas as pl
from jax.experimental.pallas import tpu as pltpu
from jax.sharding import PartitionSpec as P

CAP = 2
UNROLL = 4
MOST_PERMUTES = 16
LANES = 128
FAR = 1e30
NONE = 1 << 20
VMEM_BYTES = 67043328
VMEM_SPARE = 40 << 20

VMEM = pl.BlockSpec(memory_space=pltpu.VMEM)
SMEM = pl.BlockSpec(memory_space=pltpu.SMEM)
HBM = pl.BlockSpec(memory_space=pltpu.HBM)


def dot_nt(a, b, precision=None):
    return lax.dot_general(
        a, b, (((1,), (1,)), ((), ())), preferred_element_type=jnp.float32, precision=precision
    )


def dot_nn(a, b):
    return lax.dot_general(a, b, (((1,), (0,)), ((), ())), preferred_element_type=jnp.float32)


def dot_tn(a, b):
    return lax.dot_general(a, b, (((0,), (0,)), ((), ())), preferred_element_type=jnp.float32)


def index_kernel(shards, selected_ref, wanted_ref, bits_ref):
    head_count, block_count, pick_count = selected_ref.shape
    width = bits_ref.shape[1]
    me = lax.axis_index("seq")
    lane = lax.broadcasted_iota(jnp.int32, (block_count, width), 1)
    weight = jnp.left_shift(1, lax.broadcasted_iota(jnp.int32, (block_count, width), 0))
    for head in range(head_count):
        rows = selected_ref[head]
        hits = jnp.zeros((block_count, width), jnp.int32)
        for pick in range(pick_count):
            hits = jnp.where(rows[:, pick : pick + 1] == lane, weight, hits)
        bits_ref[head : head + 1, :] = jnp.sum(hits, axis=0, keepdims=True)
    bits = bits_ref[...]
    lane = lax.broadcasted_iota(jnp.int32, (head_count, width), 1)
    label = lax.broadcasted_iota(jnp.int32, (head_count, width), 0) * block_count + lax.rem(
        lane, block_count
    )
    label = jnp.where((bits > 0) & (lax.div(lane, block_count) != me), label, NONE)
    owner_lane = lax.div(lax.broadcasted_iota(jnp.int32, (shards, width), 1), block_count)
    mine = owner_lane == lax.broadcasted_iota(jnp.int32, (shards, width), 0)
    column = lax.broadcasted_iota(jnp.int32, (shards, LANES), 1)
    wanted = jnp.full((shards, LANES), -1, jnp.int32)
    for slot in range(CAP):
        lowest = jnp.min(label, axis=0, keepdims=True)
        slot_value = jnp.min(jnp.where(mine, lowest, NONE), axis=1, keepdims=True)
        wanted = jnp.where((column == slot) & (slot_value < NONE), slot_value, wanted)
        taken = jnp.min(jnp.where(mine, slot_value, NONE), axis=0, keepdims=True)
        label = jnp.where(label == taken, NONE, label)
    for owner in range(shards):
        wanted_ref[owner] = wanted[owner : owner + 1, :]


def gather_kernel(block_count, incoming_ref, keys_ref, values_ref, out_ref, held_ref, in_sems, out_sems):
    shards = incoming_ref.shape[0]
    head_size = out_ref.shape[2] // 2
    block_size = out_ref.shape[1] // CAP

    def fetch(owner, carry):
        for slot in range(CAP):
            unit = jnp.maximum(incoming_ref[owner, 0, slot], 0)
            head = lax.div(unit, block_count)
            block = lax.rem(unit, block_count)
            rows = pl.ds(pl.multiple_of(block * block_size, block_size), block_size)
            lanes = pl.ds(pl.multiple_of(head * head_size, head_size), head_size)
            place = slice(slot * block_size, (slot + 1) * block_size)
            for ref, half in ((keys_ref, 0), (values_ref, 1)):
                pltpu.make_async_copy(
                    ref.at[rows, lanes],
                    held_ref.at[owner, place, half * head_size : (half + 1) * head_size],
                    in_sems.at[owner],
                ).start()
        return carry

    def forward(owner, carry):
        pltpu.make_async_copy(out_ref.at[owner], held_ref.at[owner], in_sems.at[owner]).wait()
        pltpu.make_async_copy(held_ref.at[owner], out_ref.at[owner], out_sems.at[owner]).start()
        return carry

    def drain(owner, carry):
        pltpu.make_async_copy(held_ref.at[owner], out_ref.at[owner], out_sems.at[owner]).wait()
        return carry

    lax.fori_loop(0, shards, fetch, 0)
    lax.fori_loop(0, shards, forward, 0)
    lax.fori_loop(0, shards, drain, 0)


def gather_split_kernel(block_count, incoming_ref, keys_ref, values_ref, *refs):
    outs, sems = refs[:-1], refs[-1]
    shards = len(outs) + 1
    head_size = outs[0].shape[1] // 2
    block_size = outs[0].shape[0] // CAP
    me = lax.axis_index("seq")
    copies = []
    for step in range(shards - 1, 0, -1):
        asker = jnp.minimum(me + step, shards - 1)
        for slot in range(CAP):
            unit = jnp.maximum(incoming_ref[asker, 0, slot], 0)
            head = lax.div(unit, block_count)
            block = lax.rem(unit, block_count)
            rows = pl.ds(pl.multiple_of(block * block_size, block_size), block_size)
            lanes = pl.ds(pl.multiple_of(head * head_size, head_size), head_size)
            place = pl.ds(slot * block_size, block_size)
            for half, ref in enumerate((keys_ref, values_ref)):
                copy = pltpu.make_async_copy(
                    ref.at[rows, lanes],
                    outs[step - 1].at[place, pl.ds(half * head_size, head_size)],
                    sems.at[len(copies)],
                )
                copy.start()
                copies.append(copy)
    for copy in copies:
        copy.wait()


def own_kernel(
    block_count,
    bits_ref,
    q_hbm,
    k_hbm,
    v_hbm,
    o_hbm,
    do_hbm,
    lse_hbm,
    q_ref,
    do_ref,
    lse_ref,
    delta_ref,
    dq_ref,
    dk_hbm,
    dv_hbm,
    k_ref,
    v_ref,
    o_ref,
    dk_ref,
    dv_ref,
    lse_sem,
    in_sems,
    out_sems,
):
    head_count, tokens = delta_ref.shape
    head_size = q_hbm.shape[1] // head_count
    block_size = tokens // block_count
    scale = head_size ** (-0.5)
    first = lax.axis_index("seq") * block_count
    pairs = ((q_hbm, q_ref), (k_hbm, k_ref), (v_hbm, v_ref), (o_hbm, o_ref), (do_hbm, do_ref))

    def columns(head):
        return pl.ds(pl.multiple_of(head * head_size, head_size), head_size)

    def load(head, at):
        source, target = pairs[at]
        lanes = columns(head)
        return pltpu.make_async_copy(
            source.at[:, lanes], target.at[:, lanes], in_sems.at[at, head]
        )

    load_lse = pltpu.make_async_copy(lse_hbm, lse_ref, lse_sem)
    load_lse.start()

    def begin(head, carry):
        for at in range(5):
            load(head, at).start()
        return carry

    lax.fori_loop(0, head_count, begin, 0)
    load_lse.wait()
    lane_block = lax.div(lax.broadcasted_iota(jnp.int32, (1, tokens), 1), block_size)
    causal = lax.broadcasted_iota(jnp.int32, (tokens, tokens), 0) <= lax.broadcasted_iota(
        jnp.int32, (tokens, tokens), 1
    )
    ones = jnp.ones((8, 2 * head_size), jnp.bfloat16)

    def head_work(head):
        lanes = columns(head)
        q, k, v, o, do = (ref[:, lanes] for ref in (q_ref, k_ref, v_ref, o_ref, do_ref))
        product = do.astype(jnp.float32) * o.astype(jnp.float32)
        high = product.astype(jnp.bfloat16)
        rest = (product - high.astype(jnp.float32)).astype(jnp.bfloat16)
        delta = dot_nt(ones, jnp.concatenate((high, rest), axis=1))[:1]
        log_row = lse_ref[pl.ds(head, 1), :]
        rows = []
        for block in range(block_count):
            bits = bits_ref[head, first + block]
            chosen = jnp.bitwise_and(jnp.right_shift(bits, lane_block), 1) == 1
            rows.append(
                jnp.broadcast_to(jnp.where(chosen, log_row, jnp.float32(FAR)), (block_size, tokens))
            )
        shift = jnp.concatenate(rows, axis=0)
        scores = dot_nt(k, q) * scale
        probs = jnp.where(causal, jnp.exp(scores - shift), jnp.float32(0.0))
        dprobs = dot_nt(v, do)
        dscores = (probs * (dprobs - delta)).astype(jnp.bfloat16)
        dv = dot_nn(probs.astype(jnp.bfloat16), do)
        dk = dot_nn(dscores, q) * scale
        dq = dot_tn(dscores, k)
        return delta, dq, dk, dv

    def store(head, side):
        ref, out = ((dk_ref, dk_hbm), (dv_ref, dv_hbm))[side]
        lanes = columns(head)
        return pltpu.make_async_copy(ref.at[:, lanes], out.at[:, lanes], out_sems.at[side, head])

    group = 2 - head_count % 2

    def head_step(step, carry):
        heads = [step * group + at for at in range(group)]
        for head in heads:
            for at in range(5):
                load(head, at).wait()
        results = [head_work(head) for head in heads]
        for head, (delta, dq, dk, dv) in zip(heads, results):
            lanes = columns(head)
            delta_ref[pl.ds(head, 1), :] = delta
            dq_ref[:, lanes] = dq
            dk_ref[:, lanes] = dk
            dv_ref[:, lanes] = dv
            for side in range(2):
                store(head, side).start()
        return carry

    lax.fori_loop(0, head_count // group, head_step, 0)

    def drain(head, carry):
        for side in range(2):
            store(head, side).wait()
        return carry

    lax.fori_loop(0, head_count, drain, 0)


def pulled_kernel(block_count, split, shards, wanted_ref, bits_ref, *refs):
    pieces = shards - 1 if split else 1
    pulled_refs, refs = refs[:pieces], refs[pieces:]
    q_ref, do_ref, lse_ref, delta_ref, own_dq_ref, w_hbm, far_send_ref, far_keep_ref = refs[:8]
    near_send_hbm, near_keep_hbm = refs[8:10]
    grads_out, refs = refs[10 : 10 + pieces], refs[10 + pieces :]
    dq_ref, rows_ref, held_ref, grads_ref, w_ref, near_send_ref, near_keep_ref = refs[:7]
    out_sems, w_sems, near_sems = refs[7:]
    chunks = w_sems.shape[0]
    chunk = w_ref.shape[0] // chunks

    def load_w(at):
        return pltpu.make_async_copy(
            w_hbm.at[pl.ds(at * chunk, chunk)], w_ref.at[pl.ds(at * chunk, chunk)], w_sems.at[at]
        )

    def store_near(at):
        columns = pl.ds(at * chunk, chunk)
        return [
            pltpu.make_async_copy(ref.at[:, columns], out.at[:, columns], near_sems.at[side, at])
            for side, (ref, out) in enumerate(
                ((near_send_ref, near_send_hbm), (near_keep_ref, near_keep_hbm))
            )
        ]

    for at in range(chunks):
        load_w(at).start()
    tokens = q_ref.shape[0]
    head_size = grads_ref.shape[2] // 2
    block_size = grads_ref.shape[1] // CAP
    scale = head_size ** (-0.5)
    me = lax.axis_index("seq")
    lane_block = lax.div(lax.broadcasted_iota(jnp.int32, (1, tokens), 1), block_size)
    dq_ref[...] = own_dq_ref[...]
    if split:
        for at, ref in enumerate(pulled_refs):
            held_ref[at] = ref[...]
        for at in range(pieces, held_ref.shape[0]):
            held_ref[at] = jnp.zeros(held_ref.shape[1:], held_ref.dtype)
    else:
        held_ref = pulled_refs[0]

    def owner_step(step, carry):
        sums = []
        for at in range(UNROLL):
            entry = step * UNROLL + at
            owner = jnp.maximum(me - 1 - entry, 0) if split else entry
            for slot in range(CAP):
                unit = jnp.where(entry < me, wanted_ref[owner, 0, slot], -1)
                safe = jnp.maximum(unit, 0)
                head = lax.div(safe, block_count)
                block = lax.rem(safe, block_count)
                bits = jnp.where(unit >= 0, bits_ref[head, owner * block_count + block], 0)
                lanes = pl.ds(pl.multiple_of(head * head_size, head_size), head_size)
                place = slice(slot * block_size, (slot + 1) * block_size)
                q = q_ref[:, lanes]
                do = do_ref[:, lanes]
                k = held_ref[entry, place, :head_size]
                v = held_ref[entry, place, head_size:]
                chosen = jnp.bitwise_and(jnp.right_shift(bits, lane_block), 1) == 1
                shift = jnp.where(chosen, lse_ref[pl.ds(head, 1), :], jnp.float32(FAR))
                probs = jnp.exp(dot_nt(k, q) * scale - shift)
                dprobs = dot_nt(v, do)
                dscores = (probs * (dprobs - delta_ref[pl.ds(head, 1), :])).astype(jnp.bfloat16)
                dk = (dot_nn(dscores, q) * scale).astype(grads_ref.dtype)
                dv = dot_nn(probs.astype(jnp.bfloat16), do).astype(grads_ref.dtype)
                sums.append((entry, place, dk, dv, lanes, dot_tn(dscores, k)))
        for entry, place, dk, dv, lanes, value in sums:
            grads_ref[entry, place, :head_size] = dk
            grads_ref[entry, place, head_size:] = dv
            dq_ref[:, lanes] += value
        return carry

    lax.fori_loop(0, lax.div(me + UNROLL - 1, UNROLL), owner_step, 0)
    if split:
        stores = [
            pltpu.make_async_copy(grads_ref.at[at], ref, out_sems.at[at])
            for at, ref in enumerate(grads_out)
        ]
    else:
        stores = [pltpu.make_async_copy(grads_ref, grads_out[0], out_sems.at[0])]
    for store in stores:
        store.start()
    targets = (far_send_ref, far_keep_ref, near_send_ref, near_keep_ref)
    part = far_send_ref.shape[0]
    here = lax.axis_index("head")
    for place in range(4):
        start = pl.multiple_of(jnp.bitwise_xor(here, 3 - place) * part, part)
        rows_ref[place * part : (place + 1) * part, :] = (
            dq_ref[pl.ds(start, part), :] * scale
        ).astype(rows_ref.dtype)
    for at in range(chunks):
        load_w(at).wait()
        columns = slice(at * chunk, (at + 1) * chunk)
        product = dot_nt(rows_ref[...], w_ref[columns, :])
        for place, ref in enumerate(targets):
            ref[:, columns] = product[place * part : (place + 1) * part].astype(ref.dtype)
        for copy in store_near(at):
            copy.start()
    for at in range(chunks):
        for copy in store_near(at):
            copy.wait()
    for store in stores:
        store.wait()


def finish_kernel(block_count, split, incoming_ref, *refs):
    shards = incoming_ref.shape[0]
    pieces = shards - 1 if split else 1
    returned_refs = refs[:pieces]
    own_dk_hbm, own_dv_hbm, dk_out, dv_out, dk_ref, dv_ref, sems = refs[pieces:]
    head_size = returned_refs[0].shape[-1] // 2
    block_size = returned_refs[0].shape[-2] // CAP
    loads = [
        pltpu.make_async_copy(source, target, sems.at[at])
        for at, (source, target) in enumerate(
            ((own_dk_hbm, dk_ref), (own_dv_hbm, dv_ref))
        )
    ]
    for load in loads:
        load.start()
    for load in loads:
        load.wait()

    me = lax.axis_index("seq")

    def add(asker, piece):
        for slot in range(CAP):
            unit = incoming_ref[asker, 0, slot]

            @pl.when(unit >= 0)
            def _():
                head = lax.div(unit, block_count)
                block = lax.rem(unit, block_count)
                rows = pl.ds(pl.multiple_of(block * block_size, block_size), block_size)
                lanes = pl.ds(pl.multiple_of(head * head_size, head_size), head_size)
                place = slice(slot * block_size, (slot + 1) * block_size)
                dk_ref[rows, lanes] += piece[place, :head_size].astype(jnp.float32)
                dv_ref[rows, lanes] += piece[place, head_size:].astype(jnp.float32)

    if split:
        for step in range(1, shards):
            pl.when(me + step < shards)(
                functools.partial(add, jnp.minimum(me + step, shards - 1), returned_refs[step - 1])
            )
    else:

        def asker_step(asker, carry):
            add(asker, returned_refs[0].at[asker])
            return carry

        lax.fori_loop(me + 1, shards, asker_step, 0)
    dk_out[...] = dk_ref[...].astype(dk_out.dtype)
    dv_out[...] = dv_ref[...].astype(dv_out.dtype)


def per_device(queries, keys, values, outputs, out_grad, log_sum, selected, w_query):
    tokens, row_width = queries.shape
    head_count, block_count, pick_count = selected.shape
    head_size = row_width // head_count
    block_size = tokens // block_count
    shards = lax.axis_size("seq")
    groups = lax.axis_size("head")
    assert groups == 4
    width = pl.cdiv(shards * block_count, LANES) * LANES
    queries, keys, values, outputs, out_grad, log_sum, w_query = (
        pltpu.with_memory_space_constraint(a, pltpu.HBM)
        for a in (queries, keys, values, outputs, out_grad, log_sum, w_query)
    )
    f32 = jnp.float32
    bf16 = jnp.bfloat16
    shape = jax.ShapeDtypeStruct

    def params(spare=VMEM_SPARE):
        return pltpu.CompilerParams(vmem_limit_bytes=VMEM_BYTES - spare)

    def cost(flops, moved):
        return pl.CostEstimate(flops=flops, bytes_accessed=moved, transcendentals=0)

    wanted, bits = pl.pallas_call(
        functools.partial(index_kernel, shards),
        out_shape=(
            shape((shards, 1, LANES), jnp.int32),
            shape((head_count, width), jnp.int32),
        ),
        in_specs=[VMEM],
        out_specs=(VMEM, VMEM),
        compiler_params=params(),
        name="index",
    )(selected)
    incoming = lax.all_to_all(wanted, "seq", split_axis=0, concat_axis=0, tiled=True)
    exchange = (shards, CAP * block_size, 2 * head_size)
    split = shards <= MOST_PERMUTES
    piece = exchange[1:]
    pieces = shards - 1 if split else 1
    steps = range(shards - 1, 0, -1)
    if split:
        outgoing = pl.pallas_call(
            functools.partial(gather_split_kernel, block_count),
            out_shape=[shape(piece, bf16)] * pieces,
            in_specs=[SMEM, HBM, HBM],
            out_specs=[VMEM] * pieces,
            scratch_shapes=[pltpu.SemaphoreType.DMA((2 * CAP * pieces,))],
            compiler_params=params(),
            name="gather",
        )(incoming, keys, values)
        pulled = [None] * pieces
        for step in steps:
            upward = [(i, i + step) for i in range(shards - step)]
            pulled[step - 1] = lax.ppermute(outgoing[step - 1], "seq", upward)
    else:
        outgoing = pl.pallas_call(
            functools.partial(gather_kernel, block_count),
            out_shape=shape(exchange, bf16),
            in_specs=[SMEM, HBM, HBM],
            out_specs=HBM,
            scratch_shapes=[
                pltpu.VMEM(exchange, bf16),
                pltpu.SemaphoreType.DMA((shards,)),
                pltpu.SemaphoreType.DMA((shards,)),
            ],
            compiler_params=params(),
            name="gather",
        )(incoming, keys, values)
        pulled = [lax.all_to_all(outgoing, "seq", split_axis=0, concat_axis=0, tiled=True)]

    unit_flops = 10 * tokens * block_size * head_size
    q_here, do_here, lse_here, delta, own_dq, own_dk, own_dv = pl.pallas_call(
        functools.partial(own_kernel, block_count),
        out_shape=(
            shape((tokens, row_width), bf16),
            shape((tokens, row_width), bf16),
            shape((head_count, tokens), f32),
            shape((head_count, tokens), f32),
            shape((tokens, row_width), f32),
            pltpu.HBM((tokens, row_width), f32),
            pltpu.HBM((tokens, row_width), f32),
        ),
        in_specs=[SMEM] + [HBM] * 6,
        out_specs=(VMEM,) * 5 + (HBM, HBM),
        scratch_shapes=[
            pltpu.VMEM((tokens, row_width), bf16),
            pltpu.VMEM((tokens, row_width), bf16),
            pltpu.VMEM((tokens, row_width), bf16),
            pltpu.VMEM((tokens, row_width), f32),
            pltpu.VMEM((tokens, row_width), f32),
            pltpu.SemaphoreType.DMA,
            pltpu.SemaphoreType.DMA((5, head_count)),
            pltpu.SemaphoreType.DMA((2, head_count)),
        ],
        compiler_params=params(),
        cost_estimate=cost(8 * unit_flops * head_count * block_count, 22 * tokens * row_width),
        name="own",
    )(bits, queries, keys, values, outputs, out_grad, log_sum)

    part = tokens // groups
    features = w_query.shape[0]
    entries = pl.cdiv(shards, UNROLL) * UNROLL
    far_send, far_keep, near_send, near_keep, *grads = pl.pallas_call(
        functools.partial(pulled_kernel, block_count, split, shards),
        out_shape=[
            shape((part, features), bf16),
            shape((part, features), bf16),
            pltpu.HBM((part, features), bf16),
            pltpu.HBM((part, features), bf16),
        ]
        + [pltpu.HBM(piece if split else exchange, bf16)] * pieces,
        in_specs=[SMEM, SMEM] + [VMEM] * (pieces + 5) + [HBM],
        out_specs=[VMEM, VMEM] + [HBM] * (pieces + 2),
        scratch_shapes=[
            pltpu.VMEM((tokens, row_width), f32),
            pltpu.VMEM((tokens, row_width), bf16),
            pltpu.VMEM((entries if split else 1,) + piece, bf16),
            pltpu.VMEM((entries,) + piece, bf16),
            pltpu.VMEM(w_query.shape, bf16),
            pltpu.VMEM((part, features), bf16),
            pltpu.VMEM((part, features), bf16),
            pltpu.SemaphoreType.DMA((pieces,)),
            pltpu.SemaphoreType.DMA((8,)),
            pltpu.SemaphoreType.DMA((2, 8)),
        ],
        compiler_params=params(),
        cost_estimate=cost(unit_flops * shards * CAP, 10 * tokens * row_width),
        name="pulled",
    )(wanted, bits, *pulled, q_here, do_here, lse_here, delta, own_dq, w_query)

    beside = [(i, i ^ 1) for i in range(groups)]
    across = [(i, i ^ 2) for i in range(groups)]
    far_got = lax.ppermute(far_send, "head", beside)
    far_sum = (far_keep.astype(f32) + far_got.astype(f32)).astype(bf16)
    across_got = lax.ppermute(far_sum, "head", across)

    near_got = lax.ppermute(near_send, "head", beside)
    if split:
        returned = [None] * pieces
        for step in steps:
            downward = [(i + step, i) for i in range(shards - step)]
            returned[step - 1] = lax.ppermute(grads[step - 1], "seq", downward)
    else:
        returned = [lax.all_to_all(grads[0], "seq", split_axis=0, concat_axis=0, tiled=True)]
    own_dk, own_dv = (
        pltpu.with_memory_space_constraint(a, pltpu.HBM) for a in (own_dk, own_dv)
    )
    key_gradient, value_gradient = pl.pallas_call(
        functools.partial(finish_kernel, block_count, split),
        out_shape=(shape((tokens, row_width), bf16), shape((tokens, row_width), bf16)),
        in_specs=[SMEM] + [VMEM] * pieces + [HBM, HBM],
        out_specs=(VMEM, VMEM),
        scratch_shapes=[
            pltpu.VMEM((tokens, row_width), f32),
            pltpu.VMEM((tokens, row_width), f32),
            pltpu.SemaphoreType.DMA((2,)),
        ],
        compiler_params=params(),
        name="finish",
    )(incoming, *returned, own_dk, own_dv)
    x_grad = (near_keep.astype(f32) + near_got.astype(f32) + across_got.astype(f32)).astype(bf16)
    return (x_grad, key_gradient, value_gradient)


def solution(mesh):
    return jax.shard_map(
        per_device,
        mesh=mesh,
        in_specs=(
            P("seq", "head"),
            P("seq", "head"),
            P("seq", "head"),
            P("seq", "head"),
            P("seq", "head"),
            P("head", "seq"),
            P("head", "seq", None),
            P(None, "head"),
        ),
        out_specs=(P(("seq", "head"), None), P("seq", "head"), P("seq", "head")),
        check_vma=False,
    )
```

```python
import functools

import jax
import jax.numpy as jnp
from jax import lax
from jax.experimental import pallas as pl
from jax.experimental.pallas import tpu as pltpu
from jax.sharding import PartitionSpec as P


CAP = 2
UNROLL = 4
LANES = 128
FAR = 1e30
NONE = 1 << 20
VMEM_BYTES = 67043328
VMEM_SPARE = 40 << 20

VMEM = pl.BlockSpec(memory_space=pltpu.VMEM)
SMEM = pl.BlockSpec(memory_space=pltpu.SMEM)
HBM = pl.BlockSpec(memory_space=pltpu.HBM)


def dot_nt(a, b, precision=None):
    return lax.dot_general(
        a, b, (((1,), (1,)), ((), ())), preferred_element_type=jnp.float32, precision=precision
    )


def dot_nn(a, b):
    return lax.dot_general(a, b, (((1,), (0,)), ((), ())), preferred_element_type=jnp.float32)


def dot_tn(a, b):
    return lax.dot_general(a, b, (((0,), (0,)), ((), ())), preferred_element_type=jnp.float32)


def index_kernel(shards, selected_ref, wanted_ref, bits_ref):
    head_count, block_count, pick_count = selected_ref.shape
    width = bits_ref.shape[1]
    me = lax.axis_index("seq")
    lane = lax.broadcasted_iota(jnp.int32, (block_count, width), 1)
    weight = jnp.left_shift(1, lax.broadcasted_iota(jnp.int32, (block_count, width), 0))
    for head in range(head_count):
        rows = selected_ref[head]
        hits = jnp.zeros((block_count, width), jnp.int32)
        for pick in range(pick_count):
            hits = jnp.where(rows[:, pick : pick + 1] == lane, weight, hits)
        bits_ref[head : head + 1, :] = jnp.sum(hits, axis=0, keepdims=True)
    bits = bits_ref[...]
    lane = lax.broadcasted_iota(jnp.int32, (head_count, width), 1)
    label = lax.broadcasted_iota(jnp.int32, (head_count, width), 0) * block_count + lax.rem(
        lane, block_count
    )
    label = jnp.where((bits > 0) & (lax.div(lane, block_count) != me), label, NONE)
    owner_lane = lax.div(lax.broadcasted_iota(jnp.int32, (shards, width), 1), block_count)
    mine = owner_lane == lax.broadcasted_iota(jnp.int32, (shards, width), 0)
    column = lax.broadcasted_iota(jnp.int32, (shards, LANES), 1)
    wanted = jnp.full((shards, LANES), -1, jnp.int32)
    for slot in range(CAP):
        lowest = jnp.min(label, axis=0, keepdims=True)
        slot_value = jnp.min(jnp.where(mine, lowest, NONE), axis=1, keepdims=True)
        wanted = jnp.where((column == slot) & (slot_value < NONE), slot_value, wanted)
        taken = jnp.min(jnp.where(mine, slot_value, NONE), axis=0, keepdims=True)
        label = jnp.where(label == taken, NONE, label)
    for owner in range(shards):
        wanted_ref[owner] = wanted[owner : owner + 1, :]


def gather_kernel(block_count, incoming_ref, keys_ref, values_ref, out_ref, held_ref, in_sems, out_sems):
    shards = incoming_ref.shape[0]
    head_size = out_ref.shape[2] // 2
    block_size = out_ref.shape[1] // CAP

    def fetch(owner, carry):
        for slot in range(CAP):
            unit = jnp.maximum(incoming_ref[owner, 0, slot], 0)
            head = lax.div(unit, block_count)
            block = lax.rem(unit, block_count)
            rows = pl.ds(pl.multiple_of(block * block_size, block_size), block_size)
            lanes = pl.ds(pl.multiple_of(head * head_size, head_size), head_size)
            place = slice(slot * block_size, (slot + 1) * block_size)
            for ref, half in ((keys_ref, 0), (values_ref, 1)):
                pltpu.make_async_copy(
                    ref.at[rows, lanes],
                    held_ref.at[owner, place, half * head_size : (half + 1) * head_size],
                    in_sems.at[owner],
                ).start()
        return carry

    def forward(owner, carry):
        pltpu.make_async_copy(out_ref.at[owner], held_ref.at[owner], in_sems.at[owner]).wait()
        pltpu.make_async_copy(held_ref.at[owner], out_ref.at[owner], out_sems.at[owner]).start()
        return carry

    def drain(owner, carry):
        pltpu.make_async_copy(held_ref.at[owner], out_ref.at[owner], out_sems.at[owner]).wait()
        return carry

    lax.fori_loop(0, shards, fetch, 0)
    lax.fori_loop(0, shards, forward, 0)
    lax.fori_loop(0, shards, drain, 0)


def own_kernel(
    block_count,
    bits_ref,
    q_hbm,
    k_hbm,
    v_hbm,
    o_hbm,
    do_hbm,
    lse_hbm,
    q_ref,
    do_ref,
    lse_ref,
    delta_ref,
    dq_ref,
    dk_hbm,
    dv_hbm,
    k_ref,
    v_ref,
    o_ref,
    dk_ref,
    dv_ref,
    lse_sem,
    in_sems,
    out_sems,
):
    head_count, tokens = delta_ref.shape
    head_size = q_hbm.shape[1] // head_count
    block_size = tokens // block_count
    scale = head_size ** (-0.5)
    first = lax.axis_index("seq") * block_count
    pairs = ((q_hbm, q_ref), (k_hbm, k_ref), (v_hbm, v_ref), (o_hbm, o_ref), (do_hbm, do_ref))

    def columns(head):
        return pl.ds(pl.multiple_of(head * head_size, head_size), head_size)

    def load(head, at):
        source, target = pairs[at]
        lanes = columns(head)
        return pltpu.make_async_copy(
            source.at[:, lanes], target.at[:, lanes], in_sems.at[at, head]
        )

    load_lse = pltpu.make_async_copy(lse_hbm, lse_ref, lse_sem)
    load_lse.start()

    def begin(head, carry):
        for at in range(5):
            load(head, at).start()
        return carry

    lax.fori_loop(0, head_count, begin, 0)
    load_lse.wait()
    lane_block = lax.div(lax.broadcasted_iota(jnp.int32, (1, tokens), 1), block_size)
    causal = lax.broadcasted_iota(jnp.int32, (tokens, tokens), 0) <= lax.broadcasted_iota(
        jnp.int32, (tokens, tokens), 1
    )
    ones = jnp.ones((8, 2 * head_size), jnp.bfloat16)

    def head_work(head):
        lanes = columns(head)
        q, k, v, o, do = (ref[:, lanes] for ref in (q_ref, k_ref, v_ref, o_ref, do_ref))
        product = do.astype(jnp.float32) * o.astype(jnp.float32)
        high = product.astype(jnp.bfloat16)
        rest = (product - high.astype(jnp.float32)).astype(jnp.bfloat16)
        delta = dot_nt(ones, jnp.concatenate((high, rest), axis=1))[:1]
        log_row = lse_ref[pl.ds(head, 1), :]
        rows = []
        for block in range(block_count):
            bits = bits_ref[head, first + block]
            chosen = jnp.bitwise_and(jnp.right_shift(bits, lane_block), 1) == 1
            rows.append(
                jnp.broadcast_to(jnp.where(chosen, log_row, jnp.float32(FAR)), (block_size, tokens))
            )
        shift = jnp.concatenate(rows, axis=0)
        scores = dot_nt(k, q) * scale
        probs = jnp.where(causal, jnp.exp(scores - shift), jnp.float32(0.0))
        dprobs = dot_nt(v, do)
        dscores = (probs * (dprobs - delta)).astype(jnp.bfloat16)
        dv = dot_nn(probs.astype(jnp.bfloat16), do)
        dk = dot_nn(dscores, q) * scale
        dq = dot_tn(dscores, k)
        return delta, dq, dk, dv

    def store(head, side):
        ref, out = ((dk_ref, dk_hbm), (dv_ref, dv_hbm))[side]
        lanes = columns(head)
        return pltpu.make_async_copy(ref.at[:, lanes], out.at[:, lanes], out_sems.at[side, head])

    group = 2 - head_count % 2

    def head_step(step, carry):
        heads = [step * group + at for at in range(group)]
        for head in heads:
            for at in range(5):
                load(head, at).wait()
        results = [head_work(head) for head in heads]
        for head, (delta, dq, dk, dv) in zip(heads, results):
            lanes = columns(head)
            delta_ref[pl.ds(head, 1), :] = delta
            dq_ref[:, lanes] = dq
            dk_ref[:, lanes] = dk
            dv_ref[:, lanes] = dv
            for side in range(2):
                store(head, side).start()
        return carry

    lax.fori_loop(0, head_count // group, head_step, 0)

    def drain(head, carry):
        for side in range(2):
            store(head, side).wait()
        return carry

    lax.fori_loop(0, head_count, drain, 0)


def units_kernel(
    block_count,
    wanted_ref,
    bits_ref,
    pulled_ref,
    q_ref,
    do_ref,
    lse_ref,
    delta_ref,
    own_dq_ref,
    rows_ref,
    grads_hbm,
    dq_ref,
    grads_ref,
    out_sem,
):
    tokens = q_ref.shape[0]
    head_size = grads_ref.shape[2] // 2
    block_size = grads_ref.shape[1] // CAP
    scale = head_size ** (-0.5)
    lane_block = lax.div(lax.broadcasted_iota(jnp.int32, (1, tokens), 1), block_size)
    dq_ref[...] = own_dq_ref[...]

    def owner_step(step, carry):
        sums = []
        for at in range(UNROLL):
            owner = step * UNROLL + at
            for slot in range(CAP):
                unit = wanted_ref[owner, 0, slot]
                safe = jnp.maximum(unit, 0)
                head = lax.div(safe, block_count)
                block = lax.rem(safe, block_count)
                bits = jnp.where(unit >= 0, bits_ref[head, owner * block_count + block], 0)
                lanes = pl.ds(pl.multiple_of(head * head_size, head_size), head_size)
                place = slice(slot * block_size, (slot + 1) * block_size)
                q = q_ref[:, lanes]
                do = do_ref[:, lanes]
                k = pulled_ref[owner, place, :head_size]
                v = pulled_ref[owner, place, head_size:]
                chosen = jnp.bitwise_and(jnp.right_shift(bits, lane_block), 1) == 1
                shift = jnp.where(chosen, lse_ref[pl.ds(head, 1), :], jnp.float32(FAR))
                probs = jnp.exp(dot_nt(k, q) * scale - shift)
                dprobs = dot_nt(v, do)
                dscores = (probs * (dprobs - delta_ref[pl.ds(head, 1), :])).astype(jnp.bfloat16)
                dk = (dot_nn(dscores, q) * scale).astype(grads_ref.dtype)
                dv = dot_nn(probs.astype(jnp.bfloat16), do).astype(grads_ref.dtype)
                sums.append((owner, place, dk, dv, lanes, dot_tn(dscores, k)))
        for owner, place, dk, dv, lanes, value in sums:
            grads_ref[owner, place, :head_size] = dk
            grads_ref[owner, place, head_size:] = dv
            dq_ref[:, lanes] += value
        return carry

    lax.fori_loop(0, lax.div(lax.axis_index("seq") + UNROLL - 1, UNROLL), owner_step, 0)
    store = pltpu.make_async_copy(grads_ref, grads_hbm, out_sem)
    store.start()
    part = tokens // 4
    here = lax.axis_index("head")
    for place in range(4):
        start = pl.multiple_of(jnp.bitwise_xor(here, 3 - place) * part, part)
        rows_ref[place * part : (place + 1) * part, :] = (
            dq_ref[pl.ds(start, part), :] * scale
        ).astype(rows_ref.dtype)
    store.wait()


def product_kernel(rows_ref, w_hbm, *refs):
    targets, w_ref, w_sems = refs[:4], refs[4], refs[5]
    part = targets[0].shape[0]
    chunks = w_sems.shape[0]
    chunk = w_ref.shape[0] // chunks

    def load_w(at):
        rows = pl.ds(at * chunk, chunk)
        return pltpu.make_async_copy(w_hbm.at[rows], w_ref.at[rows], w_sems.at[at])

    for at in range(chunks):
        load_w(at).start()
    for at in range(chunks):
        load_w(at).wait()
        columns = slice(at * chunk, (at + 1) * chunk)
        product = dot_nt(rows_ref[...], w_ref[columns, :])
        for place, ref in enumerate(targets):
            ref[:, columns] = product[place * part : (place + 1) * part].astype(ref.dtype)


def finish_kernel(
    block_count,
    incoming_ref,
    returned_ref,
    own_dk_hbm,
    own_dv_hbm,
    dk_out,
    dv_out,
    dk_ref,
    dv_ref,
    sems,
):
    shards = incoming_ref.shape[0]
    head_size = returned_ref.shape[2] // 2
    block_size = returned_ref.shape[1] // CAP
    loads = [
        pltpu.make_async_copy(source, target, sems.at[at])
        for at, (source, target) in enumerate(
            ((own_dk_hbm, dk_ref), (own_dv_hbm, dv_ref))
        )
    ]
    for load in loads:
        load.start()
    for load in loads:
        load.wait()

    def asker_step(asker, carry):
        for slot in range(CAP):
            unit = incoming_ref[asker, 0, slot]

            @pl.when(unit >= 0)
            def _():
                head = lax.div(unit, block_count)
                block = lax.rem(unit, block_count)
                rows = pl.ds(pl.multiple_of(block * block_size, block_size), block_size)
                lanes = pl.ds(pl.multiple_of(head * head_size, head_size), head_size)
                place = slice(slot * block_size, (slot + 1) * block_size)
                dk_ref[rows, lanes] += returned_ref[asker, place, :head_size].astype(jnp.float32)
                dv_ref[rows, lanes] += returned_ref[asker, place, head_size:].astype(jnp.float32)

        return carry

    lax.fori_loop(lax.axis_index("seq") + 1, shards, asker_step, 0)
    dk_out[...] = dk_ref[...].astype(dk_out.dtype)
    dv_out[...] = dv_ref[...].astype(dv_out.dtype)


def per_device(queries, keys, values, outputs, out_grad, log_sum, selected, w_query):
    tokens, row_width = queries.shape
    head_count, block_count, _ = selected.shape
    head_size = row_width // head_count
    block_size = tokens // block_count
    shards = lax.axis_size("seq")
    groups = lax.axis_size("head")
    assert groups == 4
    width = pl.cdiv(shards * block_count, LANES) * LANES
    queries, keys, values, outputs, out_grad, log_sum, w_query = (
        pltpu.with_memory_space_constraint(a, pltpu.HBM)
        for a in (queries, keys, values, outputs, out_grad, log_sum, w_query)
    )
    f32 = jnp.float32
    bf16 = jnp.bfloat16
    shape = jax.ShapeDtypeStruct

    def params(spare=VMEM_SPARE):
        return pltpu.CompilerParams(vmem_limit_bytes=VMEM_BYTES - spare)

    def cost(flops, moved):
        return pl.CostEstimate(flops=flops, bytes_accessed=moved, transcendentals=0)

    wanted, bits = pl.pallas_call(
        functools.partial(index_kernel, shards),
        out_shape=(
            shape((shards, 1, LANES), jnp.int32),
            shape((head_count, width), jnp.int32),
        ),
        in_specs=[VMEM],
        out_specs=(VMEM, VMEM),
        compiler_params=params(),
        name="index",
    )(selected)
    incoming = lax.all_to_all(wanted, "seq", split_axis=0, concat_axis=0, tiled=True)
    exchange = (shards, CAP * block_size, 2 * head_size)
    assert shards % UNROLL == 0
    outgoing = pl.pallas_call(
        functools.partial(gather_kernel, block_count),
        out_shape=shape(exchange, bf16),
        in_specs=[SMEM, HBM, HBM],
        out_specs=HBM,
        scratch_shapes=[
            pltpu.VMEM(exchange, bf16),
            pltpu.SemaphoreType.DMA((shards,)),
            pltpu.SemaphoreType.DMA((shards,)),
        ],
        compiler_params=params(),
        name="gather",
    )(incoming, keys, values)
    pulled = lax.all_to_all(outgoing, "seq", split_axis=0, concat_axis=0, tiled=True)

    unit_flops = 10 * tokens * block_size * head_size
    q_here, do_here, lse_here, delta, own_dq, own_dk, own_dv = pl.pallas_call(
        functools.partial(own_kernel, block_count),
        out_shape=(
            shape((tokens, row_width), bf16),
            shape((tokens, row_width), bf16),
            shape((head_count, tokens), f32),
            shape((head_count, tokens), f32),
            shape((tokens, row_width), f32),
            pltpu.HBM((tokens, row_width), f32),
            pltpu.HBM((tokens, row_width), f32),
        ),
        in_specs=[SMEM] + [HBM] * 6,
        out_specs=(VMEM,) * 5 + (HBM, HBM),
        scratch_shapes=[
            pltpu.VMEM((tokens, row_width), bf16),
            pltpu.VMEM((tokens, row_width), bf16),
            pltpu.VMEM((tokens, row_width), bf16),
            pltpu.VMEM((tokens, row_width), f32),
            pltpu.VMEM((tokens, row_width), f32),
            pltpu.SemaphoreType.DMA,
            pltpu.SemaphoreType.DMA((5, head_count)),
            pltpu.SemaphoreType.DMA((2, head_count)),
        ],
        compiler_params=params(),
        cost_estimate=cost(8 * unit_flops * head_count * block_count, 22 * tokens * row_width),
        name="own",
    )(bits, queries, keys, values, outputs, out_grad, log_sum)

    part = tokens // groups
    features = w_query.shape[0]
    rows, grads = pl.pallas_call(
        functools.partial(units_kernel, block_count),
        out_shape=(shape((tokens, row_width), bf16), pltpu.HBM(exchange, bf16)),
        in_specs=[SMEM, SMEM] + [VMEM] * 6,
        out_specs=(VMEM, HBM),
        scratch_shapes=[
            pltpu.VMEM((tokens, row_width), f32),
            pltpu.VMEM(exchange, bf16),
            pltpu.SemaphoreType.DMA,
        ],
        compiler_params=params(),
        cost_estimate=cost(unit_flops * shards * CAP, 10 * tokens * row_width),
        name="units",
    )(wanted, bits, pulled, q_here, do_here, lse_here, delta, own_dq)
    returned = lax.all_to_all(grads, "seq", split_axis=0, concat_axis=0, tiled=True)

    far_send, far_keep, near_send, near_keep = pl.pallas_call(
        product_kernel,
        out_shape=(shape((part, features), bf16),) * 4,
        in_specs=[VMEM, HBM],
        out_specs=(VMEM,) * 4,
        scratch_shapes=[pltpu.VMEM(w_query.shape, bf16), pltpu.SemaphoreType.DMA((8,))],
        compiler_params=params(),
        cost_estimate=cost(8 * part * row_width * features, 2 * row_width * features),
        name="product",
    )(rows, w_query)

    beside = [(i, i ^ 1) for i in range(groups)]
    across = [(i, i ^ 2) for i in range(groups)]
    far_got = lax.ppermute(far_send, "head", beside)
    far_sum = (far_keep.astype(f32) + far_got.astype(f32)).astype(bf16)
    across_got = lax.ppermute(far_sum, "head", across)

    near_got = lax.ppermute(near_send, "head", beside)
    own_dk, own_dv = (
        pltpu.with_memory_space_constraint(a, pltpu.HBM) for a in (own_dk, own_dv)
    )
    key_gradient, value_gradient = pl.pallas_call(
        functools.partial(finish_kernel, block_count),
        out_shape=(shape((tokens, row_width), bf16), shape((tokens, row_width), bf16)),
        in_specs=[SMEM, VMEM, HBM, HBM],
        out_specs=(VMEM, VMEM),
        scratch_shapes=[
            pltpu.VMEM((tokens, row_width), f32),
            pltpu.VMEM((tokens, row_width), f32),
            pltpu.SemaphoreType.DMA((2,)),
        ],
        compiler_params=params(),
        name="finish",
    )(incoming, returned, own_dk, own_dv)
    x_grad = (near_keep.astype(f32) + near_got.astype(f32) + across_got.astype(f32)).astype(bf16)
    return (x_grad, key_gradient, value_gradient)


def solution(mesh):
    return jax.shard_map(
        per_device,
        mesh=mesh,
        in_specs=(
            P("seq", "head"),
            P("seq", "head"),
            P("seq", "head"),
            P("seq", "head"),
            P("seq", "head"),
            P("head", "seq"),
            P("head", "seq", None),
            P(None, "head"),
        ),
        out_specs=(P(("seq", "head"), None), P("seq", "head"), P("seq", "head")),
        check_vma=False,
    )
```

```python
import functools

import jax
import jax.numpy as jnp
from jax import lax
from jax.experimental import pallas as pl
from jax.experimental.pallas import tpu as pltpu
from jax.sharding import PartitionSpec as P

CAP = 2
UNROLL = 4
LANES = 128
FAR = 1e30
NONE = 1 << 20
VMEM_BYTES = 67043328
VMEM_SPARE = 40 << 20

VMEM = pl.BlockSpec(memory_space=pltpu.VMEM)
SMEM = pl.BlockSpec(memory_space=pltpu.SMEM)
HBM = pl.BlockSpec(memory_space=pltpu.HBM)


def dot_nt(a, b, precision=None):
    return lax.dot_general(
        a, b, (((1,), (1,)), ((), ())), preferred_element_type=jnp.float32, precision=precision
    )


def dot_nn(a, b):
    return lax.dot_general(a, b, (((1,), (0,)), ((), ())), preferred_element_type=jnp.float32)


def dot_tn(a, b):
    return lax.dot_general(a, b, (((0,), (0,)), ((), ())), preferred_element_type=jnp.float32)


def index_kernel(shards, selected_ref, wanted_ref, bits_ref):
    head_count, block_count, pick_count = selected_ref.shape
    width = bits_ref.shape[1]
    me = lax.axis_index("seq")
    lane = lax.broadcasted_iota(jnp.int32, (block_count, width), 1)
    weight = jnp.left_shift(1, lax.broadcasted_iota(jnp.int32, (block_count, width), 0))
    for head in range(head_count):
        rows = selected_ref[head]
        hits = jnp.zeros((block_count, width), jnp.int32)
        for pick in range(pick_count):
            hits = jnp.where(rows[:, pick : pick + 1] == lane, weight, hits)
        bits_ref[head : head + 1, :] = jnp.sum(hits, axis=0, keepdims=True)
    bits = bits_ref[...]
    lane = lax.broadcasted_iota(jnp.int32, (head_count, width), 1)
    label = lax.broadcasted_iota(jnp.int32, (head_count, width), 0) * block_count + lax.rem(
        lane, block_count
    )
    label = jnp.where((bits > 0) & (lax.div(lane, block_count) != me), label, NONE)
    owner_lane = lax.div(lax.broadcasted_iota(jnp.int32, (shards, width), 1), block_count)
    mine = owner_lane == lax.broadcasted_iota(jnp.int32, (shards, width), 0)
    column = lax.broadcasted_iota(jnp.int32, (shards, LANES), 1)
    wanted = jnp.full((shards, LANES), -1, jnp.int32)
    for slot in range(CAP):
        lowest = jnp.min(label, axis=0, keepdims=True)
        slot_value = jnp.min(jnp.where(mine, lowest, NONE), axis=1, keepdims=True)
        wanted = jnp.where((column == slot) & (slot_value < NONE), slot_value, wanted)
        taken = jnp.min(jnp.where(mine, slot_value, NONE), axis=0, keepdims=True)
        label = jnp.where(label == taken, NONE, label)
    for owner in range(shards):
        wanted_ref[owner] = wanted[owner : owner + 1, :]


def gather_kernel(block_count, incoming_ref, keys_ref, values_ref, out_ref, held_ref, in_sems, out_sems):
    shards = incoming_ref.shape[0]
    head_size = out_ref.shape[2] // 2
    block_size = out_ref.shape[1] // CAP

    def fetch(owner, carry):
        for slot in range(CAP):
            unit = jnp.maximum(incoming_ref[owner, 0, slot], 0)
            head = lax.div(unit, block_count)
            block = lax.rem(unit, block_count)
            rows = pl.ds(pl.multiple_of(block * block_size, block_size), block_size)
            lanes = pl.ds(pl.multiple_of(head * head_size, head_size), head_size)
            place = slice(slot * block_size, (slot + 1) * block_size)
            for ref, half in ((keys_ref, 0), (values_ref, 1)):
                pltpu.make_async_copy(
                    ref.at[rows, lanes],
                    held_ref.at[owner, place, half * head_size : (half + 1) * head_size],
                    in_sems.at[owner],
                ).start()
        return carry

    def forward(owner, carry):
        pltpu.make_async_copy(out_ref.at[owner], held_ref.at[owner], in_sems.at[owner]).wait()
        pltpu.make_async_copy(held_ref.at[owner], out_ref.at[owner], out_sems.at[owner]).start()
        return carry

    def drain(owner, carry):
        pltpu.make_async_copy(held_ref.at[owner], out_ref.at[owner], out_sems.at[owner]).wait()
        return carry

    lax.fori_loop(0, shards, fetch, 0)
    lax.fori_loop(0, shards, forward, 0)
    lax.fori_loop(0, shards, drain, 0)


def own_kernel(
    block_count,
    bits_ref,
    q_hbm,
    k_hbm,
    v_hbm,
    o_hbm,
    do_hbm,
    lse_hbm,
    q_ref,
    do_ref,
    lse_ref,
    delta_ref,
    dq_ref,
    dk_hbm,
    dv_hbm,
    k_ref,
    v_ref,
    o_ref,
    dk_ref,
    dv_ref,
    lse_sem,
    in_sems,
    out_sems,
):
    head_count, tokens = delta_ref.shape
    head_size = q_hbm.shape[1] // head_count
    block_size = tokens // block_count
    scale = head_size ** (-0.5)
    first = lax.axis_index("seq") * block_count
    pairs = ((q_hbm, q_ref), (k_hbm, k_ref), (v_hbm, v_ref), (o_hbm, o_ref), (do_hbm, do_ref))

    def columns(head):
        return pl.ds(pl.multiple_of(head * head_size, head_size), head_size)

    def load(head, at):
        source, target = pairs[at]
        lanes = columns(head)
        return pltpu.make_async_copy(
            source.at[:, lanes], target.at[:, lanes], in_sems.at[at, head]
        )

    load_lse = pltpu.make_async_copy(lse_hbm, lse_ref, lse_sem)
    load_lse.start()

    def begin(head, carry):
        for at in range(5):
            load(head, at).start()
        return carry

    lax.fori_loop(0, head_count, begin, 0)
    load_lse.wait()
    lane_block = lax.div(lax.broadcasted_iota(jnp.int32, (1, tokens), 1), block_size)
    causal = lax.broadcasted_iota(jnp.int32, (tokens, tokens), 0) <= lax.broadcasted_iota(
        jnp.int32, (tokens, tokens), 1
    )
    ones = jnp.ones((8, 2 * head_size), jnp.bfloat16)

    def head_work(head):
        lanes = columns(head)
        q, k, v, o, do = (ref[:, lanes] for ref in (q_ref, k_ref, v_ref, o_ref, do_ref))
        product = do.astype(jnp.float32) * o.astype(jnp.float32)
        high = product.astype(jnp.bfloat16)
        rest = (product - high.astype(jnp.float32)).astype(jnp.bfloat16)
        delta = dot_nt(ones, jnp.concatenate((high, rest), axis=1))[:1]
        log_row = lse_ref[pl.ds(head, 1), :]
        rows = []
        for block in range(block_count):
            bits = bits_ref[head, first + block]
            chosen = jnp.bitwise_and(jnp.right_shift(bits, lane_block), 1) == 1
            rows.append(
                jnp.broadcast_to(jnp.where(chosen, log_row, jnp.float32(FAR)), (block_size, tokens))
            )
        shift = jnp.concatenate(rows, axis=0)
        scores = dot_nt(k, q) * scale
        probs = jnp.where(causal, jnp.exp(scores - shift), jnp.float32(0.0))
        dprobs = dot_nt(v, do)
        dscores = (probs * (dprobs - delta)).astype(jnp.bfloat16)
        dv = dot_nn(probs.astype(jnp.bfloat16), do)
        dk = dot_nn(dscores, q) * scale
        dq = dot_tn(dscores, k)
        return delta, dq, dk, dv

    def store(head, side):
        ref, out = ((dk_ref, dk_hbm), (dv_ref, dv_hbm))[side]
        lanes = columns(head)
        return pltpu.make_async_copy(ref.at[:, lanes], out.at[:, lanes], out_sems.at[side, head])

    group = 2 - head_count % 2

    def head_step(step, carry):
        heads = [step * group + at for at in range(group)]
        for head in heads:
            for at in range(5):
                load(head, at).wait()
        results = [head_work(head) for head in heads]
        for head, (delta, dq, dk, dv) in zip(heads, results):
            lanes = columns(head)
            delta_ref[pl.ds(head, 1), :] = delta
            dq_ref[:, lanes] = dq
            dk_ref[:, lanes] = dk
            dv_ref[:, lanes] = dv
            for side in range(2):
                store(head, side).start()
        return carry

    lax.fori_loop(0, head_count // group, head_step, 0)

    def drain(head, carry):
        for side in range(2):
            store(head, side).wait()
        return carry

    lax.fori_loop(0, head_count, drain, 0)


def pulled_kernel(
    block_count,
    wanted_ref,
    bits_ref,
    pulled_ref,
    q_ref,
    do_ref,
    lse_ref,
    delta_ref,
    own_dq_ref,
    w_hbm,
    far_send_ref,
    far_keep_ref,
    near_send_hbm,
    near_keep_hbm,
    grads_hbm,
    dq_ref,
    rows_ref,
    grads_ref,
    w_ref,
    near_send_ref,
    near_keep_ref,
    out_sems,
    w_sems,
    near_sems,
):
    chunks = w_sems.shape[0]
    chunk = w_ref.shape[0] // chunks

    def load_w(at):
        rows = pl.ds(at * chunk, chunk)
        return pltpu.make_async_copy(w_hbm.at[rows], w_ref.at[rows], w_sems.at[at])

    def store_near(at):
        columns = pl.ds(at * chunk, chunk)
        return [
            pltpu.make_async_copy(ref.at[:, columns], out.at[:, columns], near_sems.at[side, at])
            for side, (ref, out) in enumerate(
                ((near_send_ref, near_send_hbm), (near_keep_ref, near_keep_hbm))
            )
        ]

    for at in range(chunks):
        load_w(at).start()
    tokens = q_ref.shape[0]
    head_size = grads_ref.shape[2] // 2
    block_size = grads_ref.shape[1] // CAP
    scale = head_size ** (-0.5)
    lane_block = lax.div(lax.broadcasted_iota(jnp.int32, (1, tokens), 1), block_size)
    dq_ref[...] = own_dq_ref[...]

    def owner_step(step, carry):
        sums = []
        for at in range(UNROLL):
            owner = step * UNROLL + at
            for slot in range(CAP):
                unit = wanted_ref[owner, 0, slot]
                safe = jnp.maximum(unit, 0)
                head = lax.div(safe, block_count)
                block = lax.rem(safe, block_count)
                bits = jnp.where(unit >= 0, bits_ref[head, owner * block_count + block], 0)
                lanes = pl.ds(pl.multiple_of(head * head_size, head_size), head_size)
                place = slice(slot * block_size, (slot + 1) * block_size)
                q = q_ref[:, lanes]
                do = do_ref[:, lanes]
                k = pulled_ref[owner, place, :head_size]
                v = pulled_ref[owner, place, head_size:]
                chosen = jnp.bitwise_and(jnp.right_shift(bits, lane_block), 1) == 1
                shift = jnp.where(chosen, lse_ref[pl.ds(head, 1), :], jnp.float32(FAR))
                probs = jnp.exp(dot_nt(k, q) * scale - shift)
                dprobs = dot_nt(v, do)
                dscores = (probs * (dprobs - delta_ref[pl.ds(head, 1), :])).astype(jnp.bfloat16)
                dk = (dot_nn(dscores, q) * scale).astype(grads_ref.dtype)
                dv = dot_nn(probs.astype(jnp.bfloat16), do).astype(grads_ref.dtype)
                sums.append((owner, place, dk, dv, lanes, dot_tn(dscores, k)))
        for owner, place, dk, dv, lanes, value in sums:
            grads_ref[owner, place, :head_size] = dk
            grads_ref[owner, place, head_size:] = dv
            dq_ref[:, lanes] += value
        store(step).start()
        return carry

    def store(step):
        owners = pl.ds(step * UNROLL, UNROLL)
        return pltpu.make_async_copy(
            grads_ref.at[owners], grads_hbm.at[owners], out_sems.at[step]
        )

    steps = lax.div(lax.axis_index("seq") + UNROLL - 1, UNROLL)
    lax.fori_loop(0, steps, owner_step, 0)
    part = tokens // 4
    here = lax.axis_index("head")
    for place in range(4):
        start = pl.multiple_of(jnp.bitwise_xor(here, 3 - place) * part, part)
        rows_ref[place * part : (place + 1) * part, :] = (
            dq_ref[pl.ds(start, part), :] * scale
        ).astype(rows_ref.dtype)
    targets = (far_send_ref, far_keep_ref, near_send_ref, near_keep_ref)
    for at in range(chunks):
        load_w(at).wait()
        columns = slice(at * chunk, (at + 1) * chunk)
        product = dot_nt(rows_ref[...], w_ref[columns, :])
        for place, ref in enumerate(targets):
            ref[:, columns] = product[place * part : (place + 1) * part].astype(ref.dtype)
        for copy in store_near(at):
            copy.start()
    for at in range(chunks):
        for copy in store_near(at):
            copy.wait()

    def drain(step, carry):
        store(step).wait()
        return carry

    lax.fori_loop(0, steps, drain, 0)


def finish_kernel(
    block_count,
    incoming_ref,
    returned_ref,
    own_dk_hbm,
    own_dv_hbm,
    dk_out,
    dv_out,
    dk_ref,
    dv_ref,
    dk_low_ref,
    dv_low_ref,
    in_sems,
    out_sems,
):
    shards = incoming_ref.shape[0]
    head_size = returned_ref.shape[2] // 2
    block_size = returned_ref.shape[1] // CAP
    groups = in_sems.shape[1]
    group = dk_ref.shape[1] // groups

    def load(at, side):
        source, target = ((own_dk_hbm, dk_ref), (own_dv_hbm, dv_ref))[side]
        lanes = pl.ds(at * group, group)
        return pltpu.make_async_copy(
            source.at[:, lanes], target.at[:, lanes], in_sems.at[side, at]
        )

    def store(at, side):
        source, target = ((dk_low_ref, dk_out), (dv_low_ref, dv_out))[side]
        lanes = pl.ds(at * group, group)
        return pltpu.make_async_copy(
            source.at[:, lanes], target.at[:, lanes], out_sems.at[side, at]
        )

    every = [(at, side) for at in range(groups) for side in range(2)]
    for at, side in every:
        load(at, side).start()
    for at, side in every:
        load(at, side).wait()

    def asker_step(asker, carry):
        for slot in range(CAP):
            unit = incoming_ref[asker, 0, slot]

            @pl.when(unit >= 0)
            def _():
                head = lax.div(unit, block_count)
                block = lax.rem(unit, block_count)
                rows = pl.ds(pl.multiple_of(block * block_size, block_size), block_size)
                lanes = pl.ds(pl.multiple_of(head * head_size, head_size), head_size)
                place = slice(slot * block_size, (slot + 1) * block_size)
                dk_ref[rows, lanes] += returned_ref[asker, place, :head_size].astype(jnp.float32)
                dv_ref[rows, lanes] += returned_ref[asker, place, head_size:].astype(jnp.float32)

        return carry

    lax.fori_loop(lax.axis_index("seq") + 1, shards, asker_step, 0)
    for at, side in every:
        lanes = slice(at * group, (at + 1) * group)
        source, target = ((dk_ref, dk_low_ref), (dv_ref, dv_low_ref))[side]
        target[:, lanes] = source[:, lanes].astype(target.dtype)
        store(at, side).start()
    for at, side in every:
        store(at, side).wait()


def per_device(queries, keys, values, outputs, out_grad, log_sum, selected, w_query):
    tokens, row_width = queries.shape
    head_count, block_count, _ = selected.shape
    head_size = row_width // head_count
    block_size = tokens // block_count
    shards = lax.axis_size("seq")
    groups = lax.axis_size("head")
    assert groups == 4
    width = pl.cdiv(shards * block_count, LANES) * LANES
    queries, keys, values, outputs, out_grad, log_sum, w_query = (
        pltpu.with_memory_space_constraint(a, pltpu.HBM)
        for a in (queries, keys, values, outputs, out_grad, log_sum, w_query)
    )
    f32 = jnp.float32
    bf16 = jnp.bfloat16
    shape = jax.ShapeDtypeStruct

    def params(spare=VMEM_SPARE):
        return pltpu.CompilerParams(vmem_limit_bytes=VMEM_BYTES - spare)

    def cost(flops, moved):
        return pl.CostEstimate(flops=flops, bytes_accessed=moved, transcendentals=0)

    wanted, bits = pl.pallas_call(
        functools.partial(index_kernel, shards),
        out_shape=(
            shape((shards, 1, LANES), jnp.int32),
            shape((head_count, width), jnp.int32),
        ),
        in_specs=[VMEM],
        out_specs=(VMEM, VMEM),
        compiler_params=params(),
        name="index",
    )(selected)
    incoming = lax.all_to_all(wanted, "seq", split_axis=0, concat_axis=0, tiled=True)
    exchange = (shards, CAP * block_size, 2 * head_size)
    assert shards % UNROLL == 0
    outgoing = pl.pallas_call(
        functools.partial(gather_kernel, block_count),
        out_shape=shape(exchange, bf16),
        in_specs=[SMEM, HBM, HBM],
        out_specs=HBM,
        scratch_shapes=[
            pltpu.VMEM(exchange, bf16),
            pltpu.SemaphoreType.DMA((shards,)),
            pltpu.SemaphoreType.DMA((shards,)),
        ],
        compiler_params=params(),
        name="gather",
    )(incoming, keys, values)
    pulled = lax.all_to_all(outgoing, "seq", split_axis=0, concat_axis=0, tiled=True)

    unit_flops = 10 * tokens * block_size * head_size
    q_here, do_here, lse_here, delta, own_dq, own_dk, own_dv = pl.pallas_call(
        functools.partial(own_kernel, block_count),
        out_shape=(
            shape((tokens, row_width), bf16),
            shape((tokens, row_width), bf16),
            shape((head_count, tokens), f32),
            shape((head_count, tokens), f32),
            shape((tokens, row_width), f32),
            pltpu.HBM((tokens, row_width), f32),
            pltpu.HBM((tokens, row_width), f32),
        ),
        in_specs=[SMEM] + [HBM] * 6,
        out_specs=(VMEM,) * 5 + (HBM, HBM),
        scratch_shapes=[
            pltpu.VMEM((tokens, row_width), bf16),
            pltpu.VMEM((tokens, row_width), bf16),
            pltpu.VMEM((tokens, row_width), bf16),
            pltpu.VMEM((tokens, row_width), f32),
            pltpu.VMEM((tokens, row_width), f32),
            pltpu.SemaphoreType.DMA,
            pltpu.SemaphoreType.DMA((5, head_count)),
            pltpu.SemaphoreType.DMA((2, head_count)),
        ],
        compiler_params=params(),
        cost_estimate=cost(8 * unit_flops * head_count * block_count, 22 * tokens * row_width),
        name="own",
    )(bits, queries, keys, values, outputs, out_grad, log_sum)

    part = tokens // groups
    features = w_query.shape[0]
    far_send, far_keep, near_send, near_keep, grads = pl.pallas_call(
        functools.partial(pulled_kernel, block_count),
        out_shape=(
            shape((part, features), bf16),
            shape((part, features), bf16),
            pltpu.HBM((part, features), bf16),
            pltpu.HBM((part, features), bf16),
            pltpu.HBM(exchange, bf16),
        ),
        in_specs=[SMEM, SMEM] + [VMEM] * 6 + [HBM],
        out_specs=(VMEM, VMEM, HBM, HBM, HBM),
        scratch_shapes=[
            pltpu.VMEM((tokens, row_width), f32),
            pltpu.VMEM((tokens, row_width), bf16),
            pltpu.VMEM(exchange, bf16),
            pltpu.VMEM(w_query.shape, bf16),
            pltpu.VMEM((part, features), bf16),
            pltpu.VMEM((part, features), bf16),
            pltpu.SemaphoreType.DMA((shards // UNROLL,)),
            pltpu.SemaphoreType.DMA((8,)),
            pltpu.SemaphoreType.DMA((2, 8)),
        ],
        compiler_params=params(),
        cost_estimate=cost(unit_flops * shards * CAP, 10 * tokens * row_width),
        name="pulled",
    )(wanted, bits, pulled, q_here, do_here, lse_here, delta, own_dq, w_query)
    returned = lax.all_to_all(grads, "seq", split_axis=0, concat_axis=0, tiled=True)

    beside = [(i, i ^ 1) for i in range(groups)]
    across = [(i, i ^ 2) for i in range(groups)]
    far_got = lax.ppermute(far_send, "head", beside)
    far_sum = (far_keep.astype(f32) + far_got.astype(f32)).astype(bf16)
    across_got = lax.ppermute(far_sum, "head", across)

    near_got = lax.ppermute(near_send, "head", beside)
    own_dk, own_dv = (
        pltpu.with_memory_space_constraint(a, pltpu.HBM) for a in (own_dk, own_dv)
    )
    key_gradient, value_gradient = pl.pallas_call(
        functools.partial(finish_kernel, block_count),
        out_shape=(shape((tokens, row_width), bf16), shape((tokens, row_width), bf16)),
        in_specs=[SMEM, VMEM, HBM, HBM],
        out_specs=(HBM, HBM),
        scratch_shapes=[
            pltpu.VMEM((tokens, row_width), f32),
            pltpu.VMEM((tokens, row_width), f32),
            pltpu.VMEM((tokens, row_width), bf16),
            pltpu.VMEM((tokens, row_width), bf16),
            pltpu.SemaphoreType.DMA((2, 4)),
            pltpu.SemaphoreType.DMA((2, 4)),
        ],
        compiler_params=params(),
        name="finish",
    )(incoming, returned, own_dk, own_dv)
    near_sum = lax.optimization_barrier(near_keep.astype(f32) + near_got.astype(f32))
    x_grad = (near_sum + across_got.astype(f32)).astype(bf16)
    return (x_grad, key_gradient, value_gradient)


def solution(mesh):
    return jax.shard_map(
        per_device,
        mesh=mesh,
        in_specs=(
            P("seq", "head"),
            P("seq", "head"),
            P("seq", "head"),
            P("seq", "head"),
            P("seq", "head"),
            P("head", "seq"),
            P("head", "seq", None),
            P(None, "head"),
        ),
        out_specs=(P(("seq", "head"), None), P("seq", "head"), P("seq", "head")),
        check_vma=False,
    )
```

```python
import functools

import jax
import jax.numpy as jnp
from jax import lax
from jax.experimental import pallas as pl
from jax.experimental.pallas import tpu as pltpu
from jax.sharding import PartitionSpec as P


CAP = 2
UNROLL = 4
PARTS = 2
LANES = 128
FAR = 1e30
NONE = 1 << 20
VMEM_BYTES = 67043328
VMEM_SPARE = 40 << 20

VMEM = pl.BlockSpec(memory_space=pltpu.VMEM)
SMEM = pl.BlockSpec(memory_space=pltpu.SMEM)
HBM = pl.BlockSpec(memory_space=pltpu.HBM)


def dot_nt(a, b, precision=None):
    return lax.dot_general(
        a, b, (((1,), (1,)), ((), ())), preferred_element_type=jnp.float32, precision=precision
    )


def dot_nn(a, b):
    return lax.dot_general(a, b, (((1,), (0,)), ((), ())), preferred_element_type=jnp.float32)


def dot_tn(a, b):
    return lax.dot_general(a, b, (((0,), (0,)), ((), ())), preferred_element_type=jnp.float32)


def index_kernel(shards, selected_ref, wanted_ref, bits_ref):
    head_count, block_count, pick_count = selected_ref.shape
    width = bits_ref.shape[1]
    me = lax.axis_index("seq")
    lane = lax.broadcasted_iota(jnp.int32, (block_count, width), 1)
    weight = jnp.left_shift(1, lax.broadcasted_iota(jnp.int32, (block_count, width), 0))
    for head in range(head_count):
        rows = selected_ref[head]
        hits = jnp.zeros((block_count, width), jnp.int32)
        for pick in range(pick_count):
            hits = jnp.where(rows[:, pick : pick + 1] == lane, weight, hits)
        bits_ref[head : head + 1, :] = jnp.sum(hits, axis=0, keepdims=True)
    bits = bits_ref[...]
    lane = lax.broadcasted_iota(jnp.int32, (head_count, width), 1)
    label = lax.broadcasted_iota(jnp.int32, (head_count, width), 0) * block_count + lax.rem(
        lane, block_count
    )
    label = jnp.where((bits > 0) & (lax.div(lane, block_count) != me), label, NONE)
    owner_lane = lax.div(lax.broadcasted_iota(jnp.int32, (shards, width), 1), block_count)
    mine = owner_lane == lax.broadcasted_iota(jnp.int32, (shards, width), 0)
    column = lax.broadcasted_iota(jnp.int32, (shards, LANES), 1)
    wanted = jnp.full((shards, LANES), -1, jnp.int32)
    for slot in range(CAP):
        lowest = jnp.min(label, axis=0, keepdims=True)
        slot_value = jnp.min(jnp.where(mine, lowest, NONE), axis=1, keepdims=True)
        wanted = jnp.where((column == slot) & (slot_value < NONE), slot_value, wanted)
        taken = jnp.min(jnp.where(mine, slot_value, NONE), axis=0, keepdims=True)
        label = jnp.where(label == taken, NONE, label)
    for owner in range(shards):
        wanted_ref[owner] = wanted[owner : owner + 1, :]


def gather_kernel(block_count, incoming_ref, keys_ref, values_ref, out_ref, held_ref, in_sems, out_sems):
    shards = incoming_ref.shape[0]
    head_size = out_ref.shape[2] // 2
    block_size = out_ref.shape[1] // CAP

    def fetch(owner, carry):
        for slot in range(CAP):
            unit = jnp.maximum(incoming_ref[owner, 0, slot], 0)
            head = lax.div(unit, block_count)
            block = lax.rem(unit, block_count)
            rows = pl.ds(pl.multiple_of(block * block_size, block_size), block_size)
            lanes = pl.ds(pl.multiple_of(head * head_size, head_size), head_size)
            place = slice(slot * block_size, (slot + 1) * block_size)
            for ref, half in ((keys_ref, 0), (values_ref, 1)):
                pltpu.make_async_copy(
                    ref.at[rows, lanes],
                    held_ref.at[owner, place, half * head_size : (half + 1) * head_size],
                    in_sems.at[owner],
                ).start()
        return carry

    def forward(owner, carry):
        pltpu.make_async_copy(out_ref.at[owner], held_ref.at[owner], in_sems.at[owner]).wait()
        pltpu.make_async_copy(held_ref.at[owner], out_ref.at[owner], out_sems.at[owner]).start()
        return carry

    def drain(owner, carry):
        pltpu.make_async_copy(held_ref.at[owner], out_ref.at[owner], out_sems.at[owner]).wait()
        return carry

    lax.fori_loop(0, shards, fetch, 0)
    lax.fori_loop(0, shards, forward, 0)
    lax.fori_loop(0, shards, drain, 0)


def own_kernel(
    block_count,
    bits_ref,
    q_hbm,
    k_hbm,
    v_hbm,
    o_hbm,
    do_hbm,
    lse_hbm,
    q_ref,
    do_ref,
    lse_ref,
    delta_ref,
    dq_ref,
    dk_hbm,
    dv_hbm,
    k_ref,
    v_ref,
    o_ref,
    dk_ref,
    dv_ref,
    lse_sem,
    in_sems,
    out_sems,
):
    head_count, tokens = delta_ref.shape
    head_size = q_hbm.shape[1] // head_count
    block_size = tokens // block_count
    scale = head_size ** (-0.5)
    first = lax.axis_index("seq") * block_count
    pairs = ((q_hbm, q_ref), (k_hbm, k_ref), (v_hbm, v_ref), (o_hbm, o_ref), (do_hbm, do_ref))

    def columns(head):
        return pl.ds(pl.multiple_of(head * head_size, head_size), head_size)

    def load(head, at):
        source, target = pairs[at]
        lanes = columns(head)
        return pltpu.make_async_copy(
            source.at[:, lanes], target.at[:, lanes], in_sems.at[at, head]
        )

    load_lse = pltpu.make_async_copy(lse_hbm, lse_ref, lse_sem)
    load_lse.start()

    def begin(head, carry):
        for at in range(5):
            load(head, at).start()
        return carry

    lax.fori_loop(0, head_count, begin, 0)
    load_lse.wait()
    lane_block = lax.div(lax.broadcasted_iota(jnp.int32, (1, tokens), 1), block_size)
    causal = lax.broadcasted_iota(jnp.int32, (tokens, tokens), 0) <= lax.broadcasted_iota(
        jnp.int32, (tokens, tokens), 1
    )
    ones = jnp.ones((8, 2 * head_size), jnp.bfloat16)

    def head_work(head):
        lanes = columns(head)
        q, k, v, o, do = (ref[:, lanes] for ref in (q_ref, k_ref, v_ref, o_ref, do_ref))
        product = do.astype(jnp.float32) * o.astype(jnp.float32)
        high = product.astype(jnp.bfloat16)
        rest = (product - high.astype(jnp.float32)).astype(jnp.bfloat16)
        delta = dot_nt(ones, jnp.concatenate((high, rest), axis=1))[:1]
        log_row = lse_ref[pl.ds(head, 1), :]
        rows = []
        for block in range(block_count):
            bits = bits_ref[head, first + block]
            chosen = jnp.bitwise_and(jnp.right_shift(bits, lane_block), 1) == 1
            rows.append(
                jnp.broadcast_to(jnp.where(chosen, log_row, jnp.float32(FAR)), (block_size, tokens))
            )
        shift = jnp.concatenate(rows, axis=0)
        scores = dot_nt(k, q) * scale
        probs = jnp.where(causal, jnp.exp(scores - shift), jnp.float32(0.0))
        dprobs = dot_nt(v, do)
        dscores = (probs * (dprobs - delta)).astype(jnp.bfloat16)
        dv = dot_nn(probs.astype(jnp.bfloat16), do)
        dk = dot_nn(dscores, q) * scale
        dq = dot_tn(dscores, k)
        return delta, dq, dk, dv

    def store(head, side):
        ref, out = ((dk_ref, dk_hbm), (dv_ref, dv_hbm))[side]
        lanes = columns(head)
        return pltpu.make_async_copy(ref.at[:, lanes], out.at[:, lanes], out_sems.at[side, head])

    group = 2 - head_count % 2

    def head_step(step, carry):
        heads = [step * group + at for at in range(group)]
        for head in heads:
            for at in range(5):
                load(head, at).wait()
        results = [head_work(head) for head in heads]
        for head, (delta, dq, dk, dv) in zip(heads, results):
            lanes = columns(head)
            delta_ref[pl.ds(head, 1), :] = delta
            dq_ref[:, lanes] = dq
            dk_ref[:, lanes] = dk
            dv_ref[:, lanes] = dv
            for side in range(2):
                store(head, side).start()
        return carry

    lax.fori_loop(0, head_count // group, head_step, 0)

    def drain(head, carry):
        for side in range(2):
            store(head, side).wait()
        return carry

    lax.fori_loop(0, head_count, drain, 0)


def units_kernel(
    block_count,
    wanted_ref,
    bits_ref,
    pulled_ref,
    q_ref,
    do_ref,
    lse_ref,
    delta_ref,
    own_dq_ref,
    rows_ref,
    grads_hbm,
    dq_ref,
    grads_ref,
    out_sem,
):
    tokens = q_ref.shape[0]
    head_size = grads_ref.shape[2] // 2
    block_size = grads_ref.shape[1] // CAP
    scale = head_size ** (-0.5)
    lane_block = lax.div(lax.broadcasted_iota(jnp.int32, (1, tokens), 1), block_size)
    dq_ref[...] = own_dq_ref[...]

    def owner_step(step, carry):
        sums = []
        for at in range(UNROLL):
            owner = step * UNROLL + at
            for slot in range(CAP):
                unit = wanted_ref[owner, 0, slot]
                safe = jnp.maximum(unit, 0)
                head = lax.div(safe, block_count)
                block = lax.rem(safe, block_count)
                bits = jnp.where(unit >= 0, bits_ref[head, owner * block_count + block], 0)
                lanes = pl.ds(pl.multiple_of(head * head_size, head_size), head_size)
                place = slice(slot * block_size, (slot + 1) * block_size)
                q = q_ref[:, lanes]
                do = do_ref[:, lanes]
                k = pulled_ref[owner, place, :head_size]
                v = pulled_ref[owner, place, head_size:]
                chosen = jnp.bitwise_and(jnp.right_shift(bits, lane_block), 1) == 1
                shift = jnp.where(chosen, lse_ref[pl.ds(head, 1), :], jnp.float32(FAR))
                probs = jnp.exp(dot_nt(k, q) * scale - shift)
                dprobs = dot_nt(v, do)
                dscores = (probs * (dprobs - delta_ref[pl.ds(head, 1), :])).astype(jnp.bfloat16)
                dk = (dot_nn(dscores, q) * scale).astype(grads_ref.dtype)
                dv = dot_nn(probs.astype(jnp.bfloat16), do).astype(grads_ref.dtype)
                sums.append((owner, place, dk, dv, lanes, dot_tn(dscores, k)))
        for owner, place, dk, dv, lanes, value in sums:
            grads_ref[owner, place, :head_size] = dk
            grads_ref[owner, place, head_size:] = dv
            dq_ref[:, lanes] += value
        return carry

    lax.fori_loop(0, lax.div(lax.axis_index("seq") + UNROLL - 1, UNROLL), owner_step, 0)
    store = pltpu.make_async_copy(grads_ref, grads_hbm, out_sem)
    store.start()
    part = tokens // 4
    here = lax.axis_index("head")
    for place in range(4):
        start = pl.multiple_of(jnp.bitwise_xor(here, 3 - place) * part, part)
        rows_ref[place * part : (place + 1) * part, :] = (
            dq_ref[pl.ds(start, part), :] * scale
        ).astype(rows_ref.dtype)
    store.wait()


def product_kernel(first, rows_ref, w_hbm, *refs):
    targets, w_ref, w_sems = refs[:4], refs[4], refs[5]
    part = targets[0].shape[0]
    chunks = w_sems.shape[0]
    chunk = w_ref.shape[0] // chunks

    def load_w(at):
        source = w_hbm.at[pl.ds(first + at * chunk, chunk)]
        return pltpu.make_async_copy(source, w_ref.at[pl.ds(at * chunk, chunk)], w_sems.at[at])

    for at in range(chunks):
        load_w(at).start()
    for at in range(chunks):
        load_w(at).wait()
        columns = slice(at * chunk, (at + 1) * chunk)
        product = dot_nt(rows_ref[...], w_ref[columns, :])
        for place, ref in enumerate(targets):
            ref[:, columns] = product[place * part : (place + 1) * part].astype(ref.dtype)


def join_kernel(*refs):
    out_ref = refs[-1]
    share = refs[0].shape[1]
    for at in range(out_ref.shape[1] // share):
        keep, got, crossed = (ref[...].astype(jnp.float32) for ref in refs[3 * at : 3 * at + 3])
        out_ref[:, at * share : (at + 1) * share] = (keep + got + crossed).astype(out_ref.dtype)


def finish_kernel(
    block_count,
    incoming_ref,
    returned_ref,
    own_dk_hbm,
    own_dv_hbm,
    dk_out,
    dv_out,
    dk_ref,
    dv_ref,
    sems,
):
    shards = incoming_ref.shape[0]
    head_size = returned_ref.shape[2] // 2
    block_size = returned_ref.shape[1] // CAP
    loads = [
        pltpu.make_async_copy(source, target, sems.at[at])
        for at, (source, target) in enumerate(
            ((own_dk_hbm, dk_ref), (own_dv_hbm, dv_ref))
        )
    ]
    for load in loads:
        load.start()
    for load in loads:
        load.wait()

    def asker_step(asker, carry):
        for slot in range(CAP):
            unit = incoming_ref[asker, 0, slot]

            @pl.when(unit >= 0)
            def _():
                head = lax.div(unit, block_count)
                block = lax.rem(unit, block_count)
                rows = pl.ds(pl.multiple_of(block * block_size, block_size), block_size)
                lanes = pl.ds(pl.multiple_of(head * head_size, head_size), head_size)
                place = slice(slot * block_size, (slot + 1) * block_size)
                dk_ref[rows, lanes] += returned_ref[asker, place, :head_size].astype(jnp.float32)
                dv_ref[rows, lanes] += returned_ref[asker, place, head_size:].astype(jnp.float32)

        return carry

    lax.fori_loop(lax.axis_index("seq") + 1, shards, asker_step, 0)
    dk_out[...] = dk_ref[...].astype(dk_out.dtype)
    dv_out[...] = dv_ref[...].astype(dv_out.dtype)


def per_device(queries, keys, values, outputs, out_grad, log_sum, selected, w_query):
    tokens, row_width = queries.shape
    head_count, block_count, _ = selected.shape
    head_size = row_width // head_count
    block_size = tokens // block_count
    shards = lax.axis_size("seq")
    groups = lax.axis_size("head")
    assert groups == 4
    width = pl.cdiv(shards * block_count, LANES) * LANES
    queries, keys, values, outputs, out_grad, log_sum, w_query = (
        pltpu.with_memory_space_constraint(a, pltpu.HBM)
        for a in (queries, keys, values, outputs, out_grad, log_sum, w_query)
    )
    f32 = jnp.float32
    bf16 = jnp.bfloat16
    shape = jax.ShapeDtypeStruct

    def params(spare=VMEM_SPARE):
        return pltpu.CompilerParams(vmem_limit_bytes=VMEM_BYTES - spare)

    def cost(flops, moved):
        return pl.CostEstimate(flops=flops, bytes_accessed=moved, transcendentals=0)

    wanted, bits = pl.pallas_call(
        functools.partial(index_kernel, shards),
        out_shape=(
            shape((shards, 1, LANES), jnp.int32),
            shape((head_count, width), jnp.int32),
        ),
        in_specs=[VMEM],
        out_specs=(VMEM, VMEM),
        compiler_params=params(),
        name="index",
    )(selected)
    incoming = lax.all_to_all(wanted, "seq", split_axis=0, concat_axis=0, tiled=True)
    exchange = (shards, CAP * block_size, 2 * head_size)
    assert shards % UNROLL == 0
    outgoing = pl.pallas_call(
        functools.partial(gather_kernel, block_count),
        out_shape=shape(exchange, bf16),
        in_specs=[SMEM, HBM, HBM],
        out_specs=HBM,
        scratch_shapes=[
            pltpu.VMEM(exchange, bf16),
            pltpu.SemaphoreType.DMA((shards,)),
            pltpu.SemaphoreType.DMA((shards,)),
        ],
        compiler_params=params(),
        name="gather",
    )(incoming, keys, values)
    pulled = lax.all_to_all(outgoing, "seq", split_axis=0, concat_axis=0, tiled=True)

    unit_flops = 10 * tokens * block_size * head_size
    q_here, do_here, lse_here, delta, own_dq, own_dk, own_dv = pl.pallas_call(
        functools.partial(own_kernel, block_count),
        out_shape=(
            shape((tokens, row_width), bf16),
            shape((tokens, row_width), bf16),
            shape((head_count, tokens), f32),
            shape((head_count, tokens), f32),
            shape((tokens, row_width), f32),
            pltpu.HBM((tokens, row_width), f32),
            pltpu.HBM((tokens, row_width), f32),
        ),
        in_specs=[SMEM] + [HBM] * 6,
        out_specs=(VMEM,) * 5 + (HBM, HBM),
        scratch_shapes=[
            pltpu.VMEM((tokens, row_width), bf16),
            pltpu.VMEM((tokens, row_width), bf16),
            pltpu.VMEM((tokens, row_width), bf16),
            pltpu.VMEM((tokens, row_width), f32),
            pltpu.VMEM((tokens, row_width), f32),
            pltpu.SemaphoreType.DMA,
            pltpu.SemaphoreType.DMA((5, head_count)),
            pltpu.SemaphoreType.DMA((2, head_count)),
        ],
        compiler_params=params(),
        cost_estimate=cost(8 * unit_flops * head_count * block_count, 22 * tokens * row_width),
        name="own",
    )(bits, queries, keys, values, outputs, out_grad, log_sum)

    part = tokens // groups
    features = w_query.shape[0]
    rows, grads = pl.pallas_call(
        functools.partial(units_kernel, block_count),
        out_shape=(shape((tokens, row_width), bf16), pltpu.HBM(exchange, bf16)),
        in_specs=[SMEM, SMEM] + [VMEM] * 6,
        out_specs=(VMEM, HBM),
        scratch_shapes=[
            pltpu.VMEM((tokens, row_width), f32),
            pltpu.VMEM(exchange, bf16),
            pltpu.SemaphoreType.DMA,
        ],
        compiler_params=params(),
        cost_estimate=cost(unit_flops * shards * CAP, 10 * tokens * row_width),
        name="units",
    )(wanted, bits, pulled, q_here, do_here, lse_here, delta, own_dq)
    returned = lax.all_to_all(grads, "seq", split_axis=0, concat_axis=0, tiled=True)

    beside = [(i, i ^ 1) for i in range(groups)]
    across = [(i, i ^ 2) for i in range(groups)]
    share = features // PARTS
    x_parts = []
    for at in range(PARTS):
        far_send, far_keep, near_send, near_keep = pl.pallas_call(
            functools.partial(product_kernel, at * share),
            out_shape=(shape((part, share), bf16),) * 4,
            in_specs=[VMEM, HBM],
            out_specs=(VMEM,) * 4,
            scratch_shapes=[pltpu.VMEM((share, row_width), bf16), pltpu.SemaphoreType.DMA((4,))],
            compiler_params=params(),
            cost_estimate=cost(8 * part * row_width * share, 2 * row_width * share),
            name="product",
        )(rows, w_query)
        far_got = lax.ppermute(far_send, "head", beside)
        far_sum = (far_keep.astype(f32) + far_got.astype(f32)).astype(bf16)
        across_got = lax.ppermute(far_sum, "head", across)
        near_got = lax.ppermute(near_send, "head", beside)
        x_parts.append((near_keep, near_got, across_got))
    own_dk, own_dv = (
        pltpu.with_memory_space_constraint(a, pltpu.HBM) for a in (own_dk, own_dv)
    )
    key_gradient, value_gradient = pl.pallas_call(
        functools.partial(finish_kernel, block_count),
        out_shape=(shape((tokens, row_width), bf16), shape((tokens, row_width), bf16)),
        in_specs=[SMEM, VMEM, HBM, HBM],
        out_specs=(VMEM, VMEM),
        scratch_shapes=[
            pltpu.VMEM((tokens, row_width), f32),
            pltpu.VMEM((tokens, row_width), f32),
            pltpu.SemaphoreType.DMA((2,)),
        ],
        compiler_params=params(),
        name="finish",
    )(incoming, returned, own_dk, own_dv)
    x_grad = pl.pallas_call(
        join_kernel,
        out_shape=shape((part, features), bf16),
        in_specs=[VMEM] * (3 * PARTS),
        out_specs=VMEM,
        compiler_params=params(),
        name="join",
    )(*[piece for pieces in x_parts for piece in pieces])
    return (x_grad, key_gradient, value_gradient)


def solution(mesh):
    return jax.shard_map(
        per_device,
        mesh=mesh,
        in_specs=(
            P("seq", "head"),
            P("seq", "head"),
            P("seq", "head"),
            P("seq", "head"),
            P("seq", "head"),
            P("head", "seq"),
            P("head", "seq", None),
            P(None, "head"),
        ),
        out_specs=(P(("seq", "head"), None), P("seq", "head"), P("seq", "head")),
        check_vma=False,
    )
```

```python
import functools

import jax
import jax.numpy as jnp
from jax import lax
from jax.experimental import pallas as pl
from jax.experimental.pallas import tpu as pltpu
from jax.sharding import PartitionSpec as P


CAP = 2
STEP_UNITS = 8
PARTS = 2
LANES = 128
FAR = 1e30
NONE = 1 << 20
VMEM_BYTES = 67043328
VMEM_SPARE = 40 << 20

VMEM = pl.BlockSpec(memory_space=pltpu.VMEM)
SMEM = pl.BlockSpec(memory_space=pltpu.SMEM)
HBM = pl.BlockSpec(memory_space=pltpu.HBM)


def dot_nt(a, b, precision=None):
    return lax.dot_general(
        a, b, (((1,), (1,)), ((), ())), preferred_element_type=jnp.float32, precision=precision
    )


def dot_nn(a, b):
    return lax.dot_general(a, b, (((1,), (0,)), ((), ())), preferred_element_type=jnp.float32)


def dot_tn(a, b):
    return lax.dot_general(a, b, (((0,), (0,)), ((), ())), preferred_element_type=jnp.float32)


def index_kernel(shards, selected_ref, wanted_ref, bits_ref):
    head_count, block_count, pick_count = selected_ref.shape
    width = bits_ref.shape[1]
    me = lax.axis_index("seq")
    lane = lax.broadcasted_iota(jnp.int32, (block_count, width), 1)
    weight = jnp.left_shift(1, lax.broadcasted_iota(jnp.int32, (block_count, width), 0))
    for head in range(head_count):
        rows = selected_ref[head]
        hits = jnp.zeros((block_count, width), jnp.int32)
        for pick in range(pick_count):
            hits = jnp.where(rows[:, pick : pick + 1] == lane, weight, hits)
        bits_ref[head : head + 1, :] = jnp.sum(hits, axis=0, keepdims=True)
    bits = bits_ref[...]
    lane = lax.broadcasted_iota(jnp.int32, (head_count, width), 1)
    label = lax.broadcasted_iota(jnp.int32, (head_count, width), 0) * block_count + lax.rem(
        lane, block_count
    )
    label = jnp.where((bits > 0) & (lax.div(lane, block_count) != me), label, NONE)
    owner_lane = lax.div(lax.broadcasted_iota(jnp.int32, (shards, width), 1), block_count)
    mine = owner_lane == lax.broadcasted_iota(jnp.int32, (shards, width), 0)
    column = lax.broadcasted_iota(jnp.int32, (shards, LANES), 1)
    wanted = jnp.full((shards, LANES), -1, jnp.int32)
    for slot in range(CAP):
        lowest = jnp.min(label, axis=0, keepdims=True)
        slot_value = jnp.min(jnp.where(mine, lowest, NONE), axis=1, keepdims=True)
        wanted = jnp.where((column == slot) & (slot_value < NONE), slot_value, wanted)
        taken = jnp.min(jnp.where(mine, slot_value, NONE), axis=0, keepdims=True)
        label = jnp.where(label == taken, NONE, label)
    for owner in range(shards):
        wanted_ref[owner] = wanted[owner : owner + 1, :]


def gather_kernel(block_count, incoming_ref, keys_ref, values_ref, out_ref, held_ref, in_sems, out_sems):
    shards = incoming_ref.shape[0]
    head_size = out_ref.shape[2] // 2
    block_size = out_ref.shape[1] // CAP

    def fetch(owner, carry):
        for slot in range(CAP):
            unit = jnp.maximum(incoming_ref[owner, 0, slot], 0)
            head = lax.div(unit, block_count)
            block = lax.rem(unit, block_count)
            rows = pl.ds(pl.multiple_of(block * block_size, block_size), block_size)
            lanes = pl.ds(pl.multiple_of(head * head_size, head_size), head_size)
            place = slice(slot * block_size, (slot + 1) * block_size)
            for ref, half in ((keys_ref, 0), (values_ref, 1)):
                pltpu.make_async_copy(
                    ref.at[rows, lanes],
                    held_ref.at[owner, place, half * head_size : (half + 1) * head_size],
                    in_sems.at[owner],
                ).start()
        return carry

    def forward(owner, carry):
        pltpu.make_async_copy(out_ref.at[owner], held_ref.at[owner], in_sems.at[owner]).wait()
        pltpu.make_async_copy(held_ref.at[owner], out_ref.at[owner], out_sems.at[owner]).start()
        return carry

    def drain(owner, carry):
        pltpu.make_async_copy(held_ref.at[owner], out_ref.at[owner], out_sems.at[owner]).wait()
        return carry

    lax.fori_loop(0, shards, fetch, 0)
    lax.fori_loop(0, shards, forward, 0)
    lax.fori_loop(0, shards, drain, 0)


def own_kernel(
    block_count,
    bits_ref,
    q_hbm,
    k_hbm,
    v_hbm,
    o_hbm,
    do_hbm,
    lse_hbm,
    q_ref,
    do_ref,
    lse_ref,
    delta_ref,
    dq_ref,
    dk_hbm,
    dv_hbm,
    k_ref,
    v_ref,
    o_ref,
    dk_ref,
    dv_ref,
    lse_sem,
    in_sems,
    out_sems,
):
    head_count, tokens = delta_ref.shape
    head_size = q_hbm.shape[1] // head_count
    block_size = tokens // block_count
    scale = head_size ** (-0.5)
    first = lax.axis_index("seq") * block_count
    pairs = ((q_hbm, q_ref), (k_hbm, k_ref), (v_hbm, v_ref), (o_hbm, o_ref), (do_hbm, do_ref))

    def columns(head):
        return pl.ds(pl.multiple_of(head * head_size, head_size), head_size)

    def load(head, at):
        source, target = pairs[at]
        lanes = columns(head)
        return pltpu.make_async_copy(
            source.at[:, lanes], target.at[:, lanes], in_sems.at[at, head]
        )

    load_lse = pltpu.make_async_copy(lse_hbm, lse_ref, lse_sem)
    load_lse.start()

    def begin(head, carry):
        for at in range(5):
            load(head, at).start()
        return carry

    lax.fori_loop(0, head_count, begin, 0)
    load_lse.wait()
    lane_block = lax.div(lax.broadcasted_iota(jnp.int32, (1, tokens), 1), block_size)
    causal = lax.broadcasted_iota(jnp.int32, (tokens, tokens), 0) <= lax.broadcasted_iota(
        jnp.int32, (tokens, tokens), 1
    )
    ones = jnp.ones((8, 2 * head_size), jnp.bfloat16)

    def head_work(head):
        lanes = columns(head)
        q, k, v, o, do = (ref[:, lanes] for ref in (q_ref, k_ref, v_ref, o_ref, do_ref))
        product = do.astype(jnp.float32) * o.astype(jnp.float32)
        high = product.astype(jnp.bfloat16)
        rest = (product - high.astype(jnp.float32)).astype(jnp.bfloat16)
        delta = dot_nt(ones, jnp.concatenate((high, rest), axis=1))[:1]
        log_row = lse_ref[pl.ds(head, 1), :]
        rows = []
        for block in range(block_count):
            bits = bits_ref[head, first + block]
            chosen = jnp.bitwise_and(jnp.right_shift(bits, lane_block), 1) == 1
            rows.append(
                jnp.broadcast_to(jnp.where(chosen, log_row, jnp.float32(FAR)), (block_size, tokens))
            )
        shift = jnp.concatenate(rows, axis=0)
        scores = dot_nt(k, q) * scale
        probs = jnp.where(causal, jnp.exp(scores - shift), jnp.float32(0.0))
        dprobs = dot_nt(v, do)
        dscores = (probs * (dprobs - delta)).astype(jnp.bfloat16)
        dv = dot_nn(probs.astype(jnp.bfloat16), do)
        dk = dot_nn(dscores, q) * scale
        dq = dot_tn(dscores, k)
        return delta, dq, dk, dv

    def store(head, side):
        ref, out = ((dk_ref, dk_hbm), (dv_ref, dv_hbm))[side]
        lanes = columns(head)
        return pltpu.make_async_copy(ref.at[:, lanes], out.at[:, lanes], out_sems.at[side, head])

    group = 2 - head_count % 2

    def head_step(step, carry):
        heads = [step * group + at for at in range(group)]
        for head in heads:
            for at in range(5):
                load(head, at).wait()
        results = [head_work(head) for head in heads]
        for head, (delta, dq, dk, dv) in zip(heads, results):
            lanes = columns(head)
            delta_ref[pl.ds(head, 1), :] = delta
            dq_ref[:, lanes] = dq
            dk_ref[:, lanes] = dk
            dv_ref[:, lanes] = dv
            for side in range(2):
                store(head, side).start()
        return carry

    lax.fori_loop(0, head_count // group, head_step, 0)

    def drain(head, carry):
        for side in range(2):
            store(head, side).wait()
        return carry

    lax.fori_loop(0, head_count, drain, 0)


def units_kernel(
    block_count,
    wanted_ref,
    bits_ref,
    pulled_ref,
    q_ref,
    do_ref,
    lse_ref,
    delta_ref,
    own_dq_ref,
    rows_ref,
    grads_hbm,
    dq_ref,
    grads_ref,
    entries_ref,
    out_sem,
):
    tokens = q_ref.shape[0]
    head_size = grads_ref.shape[2] // 2
    block_size = grads_ref.shape[1] // CAP
    scale = head_size ** (-0.5)
    lane_block = lax.div(lax.broadcasted_iota(jnp.int32, (1, tokens), 1), block_size)
    shards = wanted_ref.shape[0]
    dq_ref[...] = own_dq_ref[...]

    def collect(owner, count):
        for slot in range(CAP):
            entries_ref[count] = owner * CAP + slot
            count += (wanted_ref[owner, 0, slot] >= 0).astype(jnp.int32)
        return count

    count = lax.fori_loop(0, lax.axis_index("seq"), collect, 0)
    for at in range(STEP_UNITS):
        entries_ref[count + at] = -1

    def units_step(step, carry):
        results = []
        for at in range(STEP_UNITS):
            entry = entries_ref[step * STEP_UNITS + at]
            valid = entry >= 0
            safe = jnp.maximum(entry, 0)
            owner = lax.div(safe, CAP)
            slot = lax.rem(safe, CAP)
            unit = jnp.maximum(wanted_ref[owner, 0, slot], 0)
            head = lax.div(unit, block_count)
            block = lax.rem(unit, block_count)
            bits = jnp.where(valid, bits_ref[head, owner * block_count + block], 0)
            lanes = pl.ds(pl.multiple_of(head * head_size, head_size), head_size)
            place = pl.ds(pl.multiple_of(slot * block_size, block_size), block_size)
            q = q_ref[:, lanes]
            do = do_ref[:, lanes]
            k = pulled_ref[owner, place, :head_size]
            v = pulled_ref[owner, place, head_size:]
            chosen = jnp.bitwise_and(jnp.right_shift(bits, lane_block), 1) == 1
            shift = jnp.where(chosen, lse_ref[pl.ds(head, 1), :], jnp.float32(FAR))
            probs = jnp.exp(dot_nt(k, q) * scale - shift)
            dprobs = dot_nt(v, do)
            dscores = (probs * (dprobs - delta_ref[pl.ds(head, 1), :])).astype(jnp.bfloat16)
            dk = (dot_nn(dscores, q) * scale).astype(grads_ref.dtype)
            dv = dot_nn(probs.astype(jnp.bfloat16), do).astype(grads_ref.dtype)
            target = jnp.where(valid, owner, shards)
            results.append((target, place, dk, dv, lanes, dot_tn(dscores, k)))
        for target, place, dk, dv, lanes, value in results:
            grads_ref[target, place, :head_size] = dk
            grads_ref[target, place, head_size:] = dv
            dq_ref[:, lanes] += value
        return carry

    lax.fori_loop(0, lax.div(count + STEP_UNITS - 1, STEP_UNITS), units_step, 0)
    store = pltpu.make_async_copy(grads_ref.at[pl.ds(0, shards)], grads_hbm, out_sem)
    store.start()
    part = tokens // 4
    here = lax.axis_index("head")
    for place in range(4):
        start = pl.multiple_of(jnp.bitwise_xor(here, 3 - place) * part, part)
        rows_ref[place * part : (place + 1) * part, :] = (
            dq_ref[pl.ds(start, part), :] * scale
        ).astype(rows_ref.dtype)
    store.wait()


def product_kernel(first, rows_ref, w_hbm, *refs):
    targets, w_ref, w_sems = refs[:4], refs[4], refs[5]
    part = targets[0].shape[0]
    chunks = w_sems.shape[0]
    chunk = w_ref.shape[0] // chunks

    def load_w(at):
        source = w_hbm.at[pl.ds(first + at * chunk, chunk)]
        return pltpu.make_async_copy(source, w_ref.at[pl.ds(at * chunk, chunk)], w_sems.at[at])

    for at in range(chunks):
        load_w(at).start()
    for at in range(chunks):
        load_w(at).wait()
        columns = slice(at * chunk, (at + 1) * chunk)
        product = dot_nt(rows_ref[...], w_ref[columns, :])
        for place, ref in enumerate(targets):
            ref[:, columns] = product[place * part : (place + 1) * part].astype(ref.dtype)


def join_kernel(*refs):
    out_ref = refs[-1]
    share = refs[0].shape[1]
    for at in range(out_ref.shape[1] // share):
        keep, got, crossed = (ref[...].astype(jnp.float32) for ref in refs[3 * at : 3 * at + 3])
        out_ref[:, at * share : (at + 1) * share] = (keep + got + crossed).astype(out_ref.dtype)


def finish_kernel(
    block_count,
    incoming_ref,
    returned_ref,
    own_dk_hbm,
    own_dv_hbm,
    dk_out,
    dv_out,
    dk_ref,
    dv_ref,
    sems,
):
    shards = incoming_ref.shape[0]
    head_size = returned_ref.shape[2] // 2
    block_size = returned_ref.shape[1] // CAP
    loads = [
        pltpu.make_async_copy(source, target, sems.at[at])
        for at, (source, target) in enumerate(
            ((own_dk_hbm, dk_ref), (own_dv_hbm, dv_ref))
        )
    ]
    for load in loads:
        load.start()
    for load in loads:
        load.wait()

    def asker_step(asker, carry):
        for slot in range(CAP):
            unit = incoming_ref[asker, 0, slot]

            @pl.when(unit >= 0)
            def _():
                head = lax.div(unit, block_count)
                block = lax.rem(unit, block_count)
                rows = pl.ds(pl.multiple_of(block * block_size, block_size), block_size)
                lanes = pl.ds(pl.multiple_of(head * head_size, head_size), head_size)
                place = slice(slot * block_size, (slot + 1) * block_size)
                dk_ref[rows, lanes] += returned_ref[asker, place, :head_size].astype(jnp.float32)
                dv_ref[rows, lanes] += returned_ref[asker, place, head_size:].astype(jnp.float32)

        return carry

    lax.fori_loop(lax.axis_index("seq") + 1, shards, asker_step, 0)
    dk_out[...] = dk_ref[...].astype(dk_out.dtype)
    dv_out[...] = dv_ref[...].astype(dv_out.dtype)


def per_device(queries, keys, values, outputs, out_grad, log_sum, selected, w_query):
    tokens, row_width = queries.shape
    head_count, block_count, _ = selected.shape
    head_size = row_width // head_count
    block_size = tokens // block_count
    shards = lax.axis_size("seq")
    groups = lax.axis_size("head")
    assert groups == 4
    width = pl.cdiv(shards * block_count, LANES) * LANES
    queries, keys, values, outputs, out_grad, log_sum, w_query = (
        pltpu.with_memory_space_constraint(a, pltpu.HBM)
        for a in (queries, keys, values, outputs, out_grad, log_sum, w_query)
    )
    f32 = jnp.float32
    bf16 = jnp.bfloat16
    shape = jax.ShapeDtypeStruct

    def params(spare=VMEM_SPARE):
        return pltpu.CompilerParams(vmem_limit_bytes=VMEM_BYTES - spare)

    def cost(flops, moved):
        return pl.CostEstimate(flops=flops, bytes_accessed=moved, transcendentals=0)

    wanted, bits = pl.pallas_call(
        functools.partial(index_kernel, shards),
        out_shape=(
            shape((shards, 1, LANES), jnp.int32),
            shape((head_count, width), jnp.int32),
        ),
        in_specs=[VMEM],
        out_specs=(VMEM, VMEM),
        compiler_params=params(),
        name="index",
    )(selected)
    incoming = lax.all_to_all(wanted, "seq", split_axis=0, concat_axis=0, tiled=True)
    exchange = (shards, CAP * block_size, 2 * head_size)
    outgoing = pl.pallas_call(
        functools.partial(gather_kernel, block_count),
        out_shape=shape(exchange, bf16),
        in_specs=[SMEM, HBM, HBM],
        out_specs=HBM,
        scratch_shapes=[
            pltpu.VMEM(exchange, bf16),
            pltpu.SemaphoreType.DMA((shards,)),
            pltpu.SemaphoreType.DMA((shards,)),
        ],
        compiler_params=params(),
        name="gather",
    )(incoming, keys, values)
    pulled = lax.all_to_all(outgoing, "seq", split_axis=0, concat_axis=0, tiled=True)

    unit_flops = 10 * tokens * block_size * head_size
    q_here, do_here, lse_here, delta, own_dq, own_dk, own_dv = pl.pallas_call(
        functools.partial(own_kernel, block_count),
        out_shape=(
            shape((tokens, row_width), bf16),
            shape((tokens, row_width), bf16),
            shape((head_count, tokens), f32),
            shape((head_count, tokens), f32),
            shape((tokens, row_width), f32),
            pltpu.HBM((tokens, row_width), f32),
            pltpu.HBM((tokens, row_width), f32),
        ),
        in_specs=[SMEM] + [HBM] * 6,
        out_specs=(VMEM,) * 5 + (HBM, HBM),
        scratch_shapes=[
            pltpu.VMEM((tokens, row_width), bf16),
            pltpu.VMEM((tokens, row_width), bf16),
            pltpu.VMEM((tokens, row_width), bf16),
            pltpu.VMEM((tokens, row_width), f32),
            pltpu.VMEM((tokens, row_width), f32),
            pltpu.SemaphoreType.DMA,
            pltpu.SemaphoreType.DMA((5, head_count)),
            pltpu.SemaphoreType.DMA((2, head_count)),
        ],
        compiler_params=params(),
        cost_estimate=cost(8 * unit_flops * head_count * block_count, 22 * tokens * row_width),
        name="own",
    )(bits, queries, keys, values, outputs, out_grad, log_sum)

    part = tokens // groups
    features = w_query.shape[0]
    rows, grads = pl.pallas_call(
        functools.partial(units_kernel, block_count),
        out_shape=(shape((tokens, row_width), bf16), pltpu.HBM(exchange, bf16)),
        in_specs=[SMEM, SMEM] + [VMEM] * 6,
        out_specs=(VMEM, HBM),
        scratch_shapes=[
            pltpu.VMEM((tokens, row_width), f32),
            pltpu.VMEM((shards + 1,) + exchange[1:], bf16),
            pltpu.SMEM((shards * CAP + STEP_UNITS,), jnp.int32),
            pltpu.SemaphoreType.DMA,
        ],
        compiler_params=params(),
        cost_estimate=cost(unit_flops * shards * CAP, 10 * tokens * row_width),
        name="units",
    )(wanted, bits, pulled, q_here, do_here, lse_here, delta, own_dq)
    returned = lax.all_to_all(grads, "seq", split_axis=0, concat_axis=0, tiled=True)

    beside = [(i, i ^ 1) for i in range(groups)]
    across = [(i, i ^ 2) for i in range(groups)]
    share = features // PARTS
    x_parts = []
    for at in range(PARTS):
        far_send, far_keep, near_send, near_keep = pl.pallas_call(
            functools.partial(product_kernel, at * share),
            out_shape=(shape((part, share), bf16),) * 4,
            in_specs=[VMEM, HBM],
            out_specs=(VMEM,) * 4,
            scratch_shapes=[pltpu.VMEM((share, row_width), bf16), pltpu.SemaphoreType.DMA((4,))],
            compiler_params=params(),
            cost_estimate=cost(8 * part * row_width * share, 2 * row_width * share),
            name="product",
        )(rows, w_query)
        far_got = lax.ppermute(far_send, "head", beside)
        far_sum = (far_keep.astype(f32) + far_got.astype(f32)).astype(bf16)
        across_got = lax.ppermute(far_sum, "head", across)
        near_got = lax.ppermute(near_send, "head", beside)
        x_parts.append((near_keep, near_got, across_got))
    own_dk, own_dv = (
        pltpu.with_memory_space_constraint(a, pltpu.HBM) for a in (own_dk, own_dv)
    )
    key_gradient, value_gradient = pl.pallas_call(
        functools.partial(finish_kernel, block_count),
        out_shape=(shape((tokens, row_width), bf16), shape((tokens, row_width), bf16)),
        in_specs=[SMEM, VMEM, HBM, HBM],
        out_specs=(VMEM, VMEM),
        scratch_shapes=[
            pltpu.VMEM((tokens, row_width), f32),
            pltpu.VMEM((tokens, row_width), f32),
            pltpu.SemaphoreType.DMA((2,)),
        ],
        compiler_params=params(),
        name="finish",
    )(incoming, returned, own_dk, own_dv)
    x_grad = pl.pallas_call(
        join_kernel,
        out_shape=shape((part, features), bf16),
        in_specs=[VMEM] * (3 * PARTS),
        out_specs=VMEM,
        compiler_params=params(),
        name="join",
    )(*[piece for pieces in x_parts for piece in pieces])
    return (x_grad, key_gradient, value_gradient)


def solution(mesh):
    return jax.shard_map(
        per_device,
        mesh=mesh,
        in_specs=(
            P("seq", "head"),
            P("seq", "head"),
            P("seq", "head"),
            P("seq", "head"),
            P("seq", "head"),
            P("head", "seq"),
            P("head", "seq", None),
            P(None, "head"),
        ),
        out_specs=(P(("seq", "head"), None), P("seq", "head"), P("seq", "head")),
        check_vma=False,
    )
```
